256 devices in a mesh: section: 4 (over y), gy: 8 (over z), gx: 8 (over x, core).
Axes of the slice: x: 4, y: 4, z: 8, core: 2. Of those that a mesh axis runs over, the one named last changes fastest.
Arguments:
- level_input: bfloat16 [4, 4, 64, 128, 320], P('section', None, 'gy', 'gx'), may hold values from -72 to 72, as said below
- out_grad: bfloat16 [4, 4, 64, 128, 320], P('section', None, 'gy', 'gx'), may hold values from -6 to 6
- conv_weight: bfloat16 [4, 27, 320, 320], P('section'), may hold values from -0.0625 to 0.0625
- norm_gain: float32 [4, 320], P('section'), may hold values from 0.1 to 1.9
- norm_shift: float32 [4, 320], P('section'), may hold values from -3 to 3
Outputs:
- upstream_grad: bfloat16 [4, 4, 64, 128, 320], P('section', None, 'gy', 'gx')
- weight_grad: float32 [4, 8640, 320], P('section', ('gy', 'gx'))
- param_grad: float32 [4, 3, 320], P('section')
The draws below stay inside these ranges and needn't reach their ends.
Inputs may be any that keep to these rules, and one draw needn't show every extreme that they name: `level_input`: level input values of order one with varying channel and position scales.
All inputs are finite; a program needn't handle non-finite values.
Results may differ from the reference program's by a relative error of at most 0.0029.
Values may be sent and summed in bfloat16 or wider, within the bound.
A program may use at most 128 MiB of HBM per device.

```python
import math
import jax
import jax.numpy as jnp
from jax import lax

C = 320
G = 32
FRAMES = 4
SECTIONS = 4
HEIGHT = 64
WIDTH = 128


def draw_level_input(key, part):
    full_shape = (SECTIONS, FRAMES, HEIGHT, WIDTH, C)
    noise_key = jax.random.fold_in(key, 11)
    channel_key = jax.random.fold_in(key, 13)
    rough_key = jax.random.fold_in(key, 14)
    base_value = jnp.clip(jax.random.normal(noise_key, full_shape, jnp.float32), -4.0, 4.0)
    channel_scale = jnp.exp(jax.random.uniform(channel_key, (SECTIONS, 1, 1, 1, C), jnp.float32, math.log(0.3), math.log(3.0)))
    row_pos = jnp.arange(HEIGHT, dtype=jnp.float32) / max(HEIGHT - 1, 1)
    col_pos = jnp.arange(WIDTH, dtype=jnp.float32) / max(WIDTH - 1, 1)
    position_ramp = jnp.exp(0.5 * math.log(3.0) * (row_pos[:, None] + col_pos[None, :]))
    roughness = jnp.exp(jax.random.uniform(rough_key, (SECTIONS, FRAMES, HEIGHT, WIDTH, 1), jnp.float32, 0.0, math.log(2.0)))
    drawn = base_value * channel_scale * position_ramp[None, None, :, :, None] * roughness
    return drawn.astype(jnp.bfloat16)


def spiked(result, own_key, source, target, blocks, factor):
    def block_of(dim):
        return (jnp.arange(result.shape[dim]) // (result.shape[dim] // blocks)).reshape((-1,) + (1,) * (result.ndim - 1 - dim))

    one_side = jax.random.permutation(own_key, blocks)[block_of(target)]
    far = (block_of(target) + blocks // 2) % blocks
    return jnp.where((block_of(source) == one_side) | (block_of(source) == far), factor * result, result)


def shard_levels(key, shape, cuts, low, largest):
    def one(axis_at, parts):
        draws = jax.random.uniform(jax.random.fold_in(jax.random.fold_in(key, 6), axis_at), (parts,), jnp.float32, low / len(cuts), largest / len(cuts))
        return jnp.repeat(jnp.exp(draws), shape[axis_at] // parts).reshape((-1,) + (1,) * (len(shape) - axis_at - 1))

    level = one(*cuts[0])
    for cut in cuts[1:]:
        level = level * one(*cut)
    return level


def bell_draw(own_key, dims, deviation, limit, cuts=(), held_as=jnp.bfloat16):
    gain = shard_levels(own_key, dims, cuts, -0.22, 0.18) if cuts else 1.0
    result = jax.random.normal(own_key, dims, jnp.float32) * deviation * gain
    return jnp.minimum(jnp.maximum(result, -limit), limit).astype(held_as)


def noise_with(stream_key, dims, scale, most, cuts, heavy, kind=jnp.bfloat16):
    values = scale * jax.random.normal(stream_key, dims, jnp.float32)
    if cuts:
        values = values * shard_levels(stream_key, dims, cuts, -0.22, 0.18)
    return jnp.clip(spiked(values, jax.random.fold_in(stream_key, 3), *heavy), -most, most).astype(kind)


def setup_inputs(seed: int = 0) -> dict:
    seeds = jax.random.split(jax.random.key(seed), 6)
    level_input = draw_level_input(jax.random.fold_in(seeds[5], 71), 0)
    out_grad = noise_with(seeds[1], (SECTIONS, FRAMES, HEIGHT, WIDTH, C), 1.0, 6.0, ((0, 4), (2, 8), (3, 8)), (3, 4, 8, 2.0))
    conv_weight = bell_draw(seeds[2], (SECTIONS, 27, C, C), (27 * C) ** -0.5, 0.0625, ((0, 4),))
    norm_gain = jnp.clip(1.0 + 0.18 * jax.random.normal(seeds[3], (SECTIONS, C), jnp.float32), 0.1, 1.9)
    norm_shift = bell_draw(seeds[4], (SECTIONS, C), 0.5, 3.0, ((0, 4),), jnp.float32)
    return {"level_input": level_input, "out_grad": out_grad, "conv_weight": conv_weight, "norm_gain": norm_gain, "norm_shift": norm_shift}


eps = 1e-05

def expand_groups(values, groups, per_group):
    return jnp.broadcast_to(values[:, None], (groups, per_group)).reshape(groups * per_group)

def one_section(level_x, grad_cells, kernel_all, gain_vec, shift_vec):
    frames, height, width, channels = level_x.shape
    groups = G
    per_group = channels // groups
    cell_count = frames * height * width
    members = cell_count * per_group
    x_float = level_x.astype(jnp.float32).reshape(cell_count, groups, per_group)
    group_mean = lax.optimization_barrier(jnp.sum(x_float, axis=(0, 2))) / members
    centered = x_float - group_mean[None, :, None]
    group_var = lax.optimization_barrier(jnp.sum(centered * centered, axis=(0, 2))) / members
    inv_std = 1.0 / jnp.sqrt(group_var + eps)
    normed = (centered * inv_std[None, :, None]).reshape(cell_count, channels)
    activ = normed * gain_vec[None, :] + shift_vec[None, :]
    sigmoid_v = jax.nn.sigmoid(activ)
    unit_rows = (activ * sigmoid_v).astype(jnp.bfloat16)
    framed = jnp.pad(grad_cells, ((1, 1), (1, 1), (1, 1), (0, 0)))
    weight_pieces = []
    input_side = jnp.zeros((cell_count, channels), jnp.float32)
    for offset_f in range(3):
        for offset_h in range(3):
            for offset_w in range(3):
                kernel_idx = offset_f * 9 + offset_h * 3 + offset_w
                window = framed[2 - offset_f:2 - offset_f + frames, 2 - offset_h:2 - offset_h + height, 2 - offset_w:2 - offset_w + width, :].reshape(cell_count, channels)
                weight_pieces.append(lax.dot_general(unit_rows, window, (((0,), (0,)), ((), ())), preferred_element_type=jnp.float32))
                input_side = input_side + lax.dot_general(window, kernel_all[kernel_idx], (((1,), (1,)), ((), ())), preferred_element_type=jnp.float32)
    silu_slope = sigmoid_v * (1.0 + activ * (1.0 - sigmoid_v))
    act_grad = input_side * silu_slope
    grad_float = grad_cells.astype(jnp.float32).reshape(cell_count, channels)
    gain_sum = lax.optimization_barrier(jnp.sum(act_grad * normed, axis=0))
    shift_sum = lax.optimization_barrier(jnp.sum(act_grad, axis=0))
    bias_sum = lax.optimization_barrier(jnp.sum(grad_float, axis=0))
    mean_first = lax.optimization_barrier(jnp.sum((gain_vec * shift_sum).reshape(groups, per_group), axis=1)) / members
    mean_second = lax.optimization_barrier(jnp.sum((gain_vec * gain_sum).reshape(groups, per_group), axis=1)) / members
    norm_grad = (act_grad * gain_vec[None, :] - expand_groups(mean_first, groups, per_group)[None, :] - normed * expand_groups(mean_second, groups, per_group)[None, :]) * expand_groups(inv_std, groups, per_group)[None, :]
    level_grad = (grad_float + norm_grad).astype(jnp.bfloat16).reshape(frames, height, width, channels)
    weight_grad = jnp.concatenate(weight_pieces, axis=0)
    param_grad = jnp.stack([gain_sum, shift_sum, bias_sum])
    return (level_grad, weight_grad, param_grad)

def reference(level_input, out_grad, conv_weight, norm_gain, norm_shift):
    section_count = level_input.shape[0]
    level_list = []
    weight_list = []
    param_list = []
    for section_idx in range(section_count):
        level_grad, weight_grad, param_grad = one_section(level_input[section_idx], out_grad[section_idx], conv_weight[section_idx], norm_gain[section_idx], norm_shift[section_idx])
        level_list.append(level_grad)
        weight_list.append(weight_grad)
        param_list.append(param_grad)
    upstream_grad = jnp.stack(level_list[1:] + [jnp.zeros_like(level_list[0])])
    return (upstream_grad, jnp.stack(weight_list), jnp.stack(param_list))
```

```python
import functools

import jax
import jax.numpy as jnp
from jax import lax
from jax.experimental import pallas as pl
from jax.experimental.pallas import tpu as pltpu
from jax.sharding import PartitionSpec as P

G = 32
EPS = 1e-05
MESH = pl.DeviceIdType.MESH
SUB = 5
SLAB = 1080
ROWS = SLAB // SUB
F32 = jnp.float32
BF16 = jnp.bfloat16


def kernel(x_ref, g_ref, w_hbm, gain_ref, shift_ref, grp_ref,
           up_ref, dw_ref, par_ref,
           wbuf, gs, pgs, gf, tmp, edge_out, edge_l, edge_r,
           st_x, rx_sx, st_z, rx_sz, pa_x, rx_px, pa_z, rx_pz,
           unit_own, unit_par, unit_t, acc, normed_b, slope_b, part,
           sbuf, ra, rb, fsend, frecv, lsend, lrecv,
           wsem, zsem, zrsem, esem, ersem, gsem, grsem, usem, ursem,
           sxs, sxr, szs, szr, pxs, pxr, pzs, pzr,
           ssem, rasem, rbsem, fsem, frsem, ysem, yrsem):
    s = lax.axis_index("section")
    z = lax.axis_index("gy")
    me = lax.axis_index("gx")
    core = me % 2
    xc = me // 2
    partner = xc * 2 + 1 - core

    wcopy = pltpu.make_async_copy(w_hbm, wbuf, wsem)
    wcopy.start()

    barrier = pltpu.get_barrier_semaphore()
    for d in range(1, 8):
        pl.semaphore_signal(barrier, inc=1, device_id={"gx": (me + d) % 8}, device_id_type=MESH)
        pl.semaphore_signal(barrier, inc=1, device_id={"gy": (z + d) % 8}, device_id_type=MESH)

    @pl.when(s > 0)
    def _():
        pl.semaphore_signal(barrier, inc=1, device_id={"section": s - 1}, device_id_type=MESH)

    @pl.when(s < 3)
    def _():
        pl.semaphore_signal(barrier, inc=1, device_id={"section": s + 1}, device_id_type=MESH)

    def stat_body(i, carry):
        a, b = carry
        v = x_ref[pl.ds(pl.multiple_of(i * 64, 64), 64), :].astype(F32)
        return a + jnp.sum(v.reshape(8, 8, 320), axis=0), b + jnp.sum((v * v).reshape(8, 8, 320), axis=0)

    zero8 = jnp.zeros((8, 320), F32)
    a, b = lax.fori_loop(0, 8, stat_body, (zero8, zero8))
    st_x[...] = zero8
    st_x[0:1, :] = jnp.sum(a, axis=0, keepdims=True)
    st_x[1:2, :] = jnp.sum(b, axis=0, keepdims=True)

    first_entry = 14 + jnp.where(s > 0, 1, 0) + jnp.where(s < 3, 1, 0)
    pl.semaphore_wait(barrier, first_entry)

    def gather(src, dst, ssems, rsems, axis, at):
        out = []
        for d in range(1, 8):
            to = (at + d) % 8
            out.append(pltpu.make_async_remote_copy(
                src_ref=src, dst_ref=dst.at[at], send_sem=ssems.at[d], recv_sem=rsems.at[at],
                device_id={axis: to}, device_id_type=MESH))
            out[-1].start()
        dst[pl.ds(at, 1)] = src[...][None]

    def gathered(src, dst, ssems, rsems, axis, at):
        for d in range(1, 8):
            frm = (at + d) % 8
            cp = pltpu.make_async_remote_copy(
                src_ref=src, dst_ref=dst.at[frm], send_sem=ssems.at[d], recv_sem=rsems.at[frm],
                device_id={axis: frm}, device_id_type=MESH)
            cp.wait_send()
            cp.wait_recv()
        tot = dst[0]
        for d in range(1, 8):
            tot = tot + dst[d]
        return tot

    def halo(src_row, dst_row, to, i):
        return pltpu.make_async_remote_copy(
            src_ref=g_ref.at[:, pl.ds(src_row, 16), :],
            dst_ref=gs.at[1, pl.ds(1, 4), pl.ds(dst_row, 16), :],
            send_sem=zsem.at[i], recv_sem=zrsem.at[i], device_id={"gy": to}, device_id_type=MESH)

    up_halo = halo(0, 144, jnp.maximum(z - 1, 0), 0)
    down_halo = halo(112, 0, jnp.minimum(z + 1, 7), 1)
    pl.when(z > 0)(lambda: up_halo.start())
    pl.when(z < 7)(lambda: down_halo.start())
    gather(st_x, rx_sx, sxs, sxr, "gx", me)

    zrow = jnp.zeros((4, 16, 320), BF16)
    for c in range(3):
        gs[c, 0] = jnp.zeros((160, 320), BF16)
        gs[c, 5] = jnp.zeros((160, 320), BF16)

    @pl.when(z == 0)
    def _():
        gs[1, 1:5, 0:16, :] = zrow

    @pl.when(z == 7)
    def _():
        gs[1, 1:5, 144:160, :] = zrow

    bsum = jnp.zeros((1, 320), F32)
    for f in range(4):
        v = g_ref[f]
        gs[1, 1 + f, 16:144, :] = v
        v = v.astype(F32)
        bsum = bsum + jnp.sum(v, axis=0, keepdims=True)
    pa_x[...] = zero8
    pa_x[2:3, :] = bsum

    @pl.when(z > 0)
    def _():
        up_halo.wait_send()
        down_halo.wait_recv()

    @pl.when(z < 7)
    def _():
        down_halo.wait_send()
        up_halo.wait_recv()

    for f in range(4):
        v = gs[1, 1 + f].astype(F32)
        gf[f, 0] = v[:, 0:128]
        gf[f, 1] = v[:, 128:256]
        gf[f, 2] = jnp.concatenate([v[:, 256:320], jnp.zeros((160, 64), F32)], axis=1)
    for f in range(4):
        for l in range(3):
            edge_out[0, f, l] = jnp.zeros((16, 128), F32)
            edge_out[1, f, l] = jnp.zeros((16, 128), F32)
            edge_out[0, f, l, 0:10, :] = gf[f, l, pl.ds(0, 10, stride=16), :]
            edge_out[1, f, l, 0:10, :] = gf[f, l, pl.ds(15, 10, stride=16), :]
    to_left = pltpu.make_async_remote_copy(
        src_ref=edge_out.at[0], dst_ref=edge_r, send_sem=esem.at[0], recv_sem=ersem.at[0],
        device_id={"gx": jnp.maximum(me - 1, 0)}, device_id_type=MESH)
    to_right = pltpu.make_async_remote_copy(
        src_ref=edge_out.at[1], dst_ref=edge_l, send_sem=esem.at[1], recv_sem=ersem.at[1],
        device_id={"gx": jnp.minimum(me + 1, 7)}, device_id_type=MESH)
    pl.when(me > 0)(lambda: to_left.start())
    pl.when(me < 7)(lambda: to_right.start())

    @pl.when(me == 0)
    def _():
        edge_l[...] = jnp.zeros((4, 3, 16, 128), F32)

    @pl.when(me == 7)
    def _():
        edge_r[...] = jnp.zeros((4, 3, 16, 128), F32)

    st_z[...] = gathered(st_x, rx_sx, sxs, sxr, "gx", me)
    gather(st_z, rx_sz, szs, szr, "gy", z)

    @pl.when(me > 0)
    def _():
        to_left.wait_send()
        to_right.wait_recv()

    @pl.when(me < 7)
    def _():
        to_right.wait_send()
        to_left.wait_recv()

    for f in range(4):
        for l in range(3):
            w = 128 if l < 2 else 64
            v = gf[f, l]
            tmp[0] = pltpu.roll(v, 1, 0)
            tmp[1] = pltpu.roll(v, 159, 0)
            tmp[0, pl.ds(0, 10, stride=16), :] = edge_l[f, l, 0:10, :]
            tmp[1, pl.ds(15, 10, stride=16), :] = edge_r[f, l, 0:10, :]
            gs[2, 1 + f, :, 128 * l:128 * l + w] = tmp[0, :, 0:w].astype(BF16)
            gs[0, 1 + f, :, 128 * l:128 * l + w] = tmp[1, :, 0:w].astype(BF16)
    swap = pltpu.make_async_remote_copy(
        src_ref=gs, dst_ref=pgs, send_sem=gsem, recv_sem=grsem,
        device_id={"gx": partner}, device_id_type=MESH)
    swap.start()

    wcopy.wait()

    def window(ref, c, a, b):
        v = ref[c, pl.ds(2 - a, 4), pl.ds(pl.multiple_of((2 - b) * 16, 16), 128), :]
        return v.reshape(512, 320)

    def side(ab, first):
        a, b = ab // 3, ab % 3
        tot = None
        for c in range(3):
            wk = wbuf[ab * 3 + c]
            d = lax.dot_general(window(gs, c, a, b), wk, (((1,), (1,)), ((), ())), preferred_element_type=F32)
            tot = d if tot is None else tot + d
        acc[...] += tot
        return first

    acc[...] = jnp.zeros((512, 320), F32)
    lax.fori_loop(0, 9, side, 0)

    tot = gathered(st_z, rx_sz, szs, szr, "gy", z)
    members = float(512 * 64 * 10)
    grp = grp_ref[...]
    per = jnp.dot(tot, grp, precision=lax.Precision.HIGHEST, preferred_element_type=F32) / members
    mean = per[0:1, :]
    var = per[1:2, :] - mean * mean
    inv = 1.0 / jnp.sqrt(var + EPS)
    gain = gain_ref[...]
    shift = shift_ref[...]

    def act_body(i, carry):
        p0, p1 = carry
        rows = pl.ds(pl.multiple_of(i * 32, 32), 32)
        n = (x_ref[rows, :].astype(F32) - mean) * inv
        y = n * gain + shift
        sg = jax.nn.sigmoid(y)
        unit_own[rows, :] = (y * sg).astype(BF16)
        ag = acc[rows, :] * (sg * (1.0 + y * (1.0 - sg)))
        acc[rows, :] = ag
        normed_b[rows, :] = n
        return p0 + jnp.sum((ag * n).reshape(4, 8, 320), axis=0), p1 + jnp.sum(ag.reshape(4, 8, 320), axis=0)

    p0, p1 = lax.fori_loop(0, 16, act_body, (zero8, zero8))
    swap_u = pltpu.make_async_remote_copy(
        src_ref=unit_own, dst_ref=unit_par, send_sem=usem, recv_sem=ursem,
        device_id={"gx": partner}, device_id_type=MESH)
    swap_u.start()
    pa_x[0:1, :] = jnp.sum(p0, axis=0, keepdims=True)
    pa_x[1:2, :] = jnp.sum(p1, axis=0, keepdims=True)
    gather(pa_x, rx_px, pxs, pxr, "gx", me)

    unit_t[:, 0:512] = unit_own[...].T
    swap.wait()
    swap_u.wait()
    unit_t[:, 512:1024] = unit_par[...].T
    pa_z[...] = gathered(pa_x, rx_px, pxs, pxr, "gx", me)
    gather(pa_z, rx_pz, pzs, pzr, "gy", z)

    def taps(t, carry):
        k = 13 * core + t
        ab = k // 3
        c = k % 3
        a, b = ab // 3, ab % 3
        win = jnp.concatenate([window(gs, c, a, b), window(pgs, c, a, b)], axis=0)
        part[pl.ds(pl.multiple_of(t * 320, 64), 320), :] = jnp.dot(unit_t[...], win, preferred_element_type=F32)
        return carry

    lax.fori_loop(0, 14, taps, 0)

    def base_of(j):
        return pl.multiple_of(160 * core + SLAB * j, 8)

    def hop(j, i, up):
        to = jnp.where(up, z + 1, z + 7) % 8
        return to

    def step(tau, carry):
        def one(j, c2):
            delta = (4 * core + j - z + 8) % 8
            for i in range(SUB):
                top = 4 - (i % 2)
                going_up = (delta >= 1) & (delta <= top)
                going_down = delta > top
                when_up = top - delta
                when_down = delta - top - 1
                rows = pl.ds(pl.multiple_of(base_of(j) + ROWS * i, 8), ROWS)

                def sends_up(j=j, i=i):
                    return pltpu.make_async_remote_copy(
                        src_ref=sbuf.at[j, i], dst_ref=ra.at[j, i], send_sem=ssem.at[j, i],
                        recv_sem=rasem.at[j, i], device_id={"gy": (z + 1) % 8}, device_id_type=MESH)

                def sends_down(j=j, i=i):
                    return pltpu.make_async_remote_copy(
                        src_ref=sbuf.at[j, i], dst_ref=rb.at[j, i], send_sem=ssem.at[j, i],
                        recv_sem=rbsem.at[j, i], device_id={"gy": (z + 7) % 8}, device_id_type=MESH)

                @pl.when(going_up & (when_up == tau))
                def _():
                    @pl.when(tau == 0)
                    def _():
                        sbuf[j, i] = part[rows, :].astype(BF16)

                    @pl.when(tau > 0)
                    def _():
                        sends_up().wait_recv()
                        sbuf[j, i] = (part[rows, :] + ra[j, i].astype(F32)).astype(BF16)

                    sends_up().start()

                @pl.when(going_down & (when_down == tau))
                def _():
                    @pl.when(tau == 0)
                    def _():
                        sbuf[j, i] = part[rows, :].astype(BF16)

                    @pl.when(tau > 0)
                    def _():
                        sends_down().wait_recv()
                        sbuf[j, i] = (part[rows, :] + rb[j, i].astype(F32)).astype(BF16)

                    sends_down().start()

                @pl.when((delta == 0) & (tau == 4))
                def _():
                    sends_up().wait_recv()
                    sends_down().wait_recv()
                    part[rows, :] = part[rows, :] + ra[j, i].astype(F32) + rb[j, i].astype(F32)

            return c2

        lax.fori_loop(0, 4, one, 0)
        return carry

    step(0, 0)

    ptot = gathered(pa_z, rx_pz, pzs, pzr, "gy", z)
    par_ref[...] = ptot[0:3, :]
    gg = jnp.dot(ptot * gain, grp, precision=lax.Precision.HIGHEST, preferred_element_type=F32) / members
    second = gg[0:1, :]
    first = gg[1:2, :]

    def lev(i, carry):
        rows = pl.ds(pl.multiple_of(i * 32, 32), 32)
        gv = g_ref[i // 4, pl.ds(pl.multiple_of((i % 4) * 32, 32), 32), :].astype(F32)
        ng = (acc[rows, :] * gain - first - normed_b[rows, :] * second) * inv
        lsend[rows, :] = (gv + ng).astype(BF16)
        return carry

    lax.fori_loop(0, 16, lev, 0)
    ycopy = pltpu.make_async_remote_copy(
        src_ref=lsend, dst_ref=lrecv, send_sem=ysem, recv_sem=yrsem,
        device_id={"section": jnp.maximum(s - 1, 0)}, device_id_type=MESH)
    pl.when(s > 0)(lambda: ycopy.start())

    lax.fori_loop(1, 5, step, 0)

    root = z // 4

    @pl.when(core == root)
    def _():
        j = z - 4 * core
        for d in range(8):
            lo = (135 * d) // 8 * 8
            v = part[pl.ds(pl.multiple_of(base_of(j) + lo, 8), 144 if d < 7 else 136), :]
            fsend[d, 0:135, :] = v[135 * d - lo:135 * d - lo + 135, :]
        for d in range(1, 8):
            to = (me + d) % 8
            pltpu.make_async_remote_copy(
                src_ref=fsend.at[to], dst_ref=frecv.at[xc], send_sem=fsem.at[d], recv_sem=frsem.at[xc],
                device_id={"gx": to}, device_id_type=MESH).start()
        frecv[pl.ds(xc, 1)] = fsend[pl.ds(me, 1)]

    for q in range(4):
        src = 2 * q + root

        @pl.when(src != me)
        def _(q=q):
            pltpu.make_async_remote_copy(
                src_ref=fsend.at[q], dst_ref=frecv.at[q], send_sem=fsem.at[0], recv_sem=frsem.at[q],
                device_id={"gx": partner}, device_id_type=MESH).wait_recv()

    tot = frecv[0, 0:135, :]
    for q in range(1, 4):
        tot = tot + frecv[q, 0:135, :]
    dw_ref[...] = tot

    @pl.when(core == root)
    def _():
        for d in range(1, 8):
            pltpu.make_async_remote_copy(
                src_ref=fsend.at[d], dst_ref=frecv.at[0], send_sem=fsem.at[d], recv_sem=frsem.at[0],
                device_id={"gx": (me + d) % 8}, device_id_type=MESH).wait_send()

    def drain(j, carry):
        delta = (4 * core + j - z + 8) % 8

        @pl.when(delta != 0)
        def _():
            for i in range(SUB):
                pltpu.make_async_remote_copy(
                    src_ref=sbuf.at[j, i], dst_ref=ra.at[j, i], send_sem=ssem.at[j, i],
                    recv_sem=rasem.at[j, i], device_id={"gy": (z + 1) % 8}, device_id_type=MESH).wait_send()

        return carry

    lax.fori_loop(0, 4, drain, 0)
    pl.when(s > 0)(lambda: ycopy.wait_send())

    @pl.when(s < 3)
    def _():
        ycopy.wait_recv()
        up_ref[...] = lrecv[...]

    @pl.when(s == 3)
    def _():
        up_ref[...] = jnp.zeros((512, 320), BF16)


def local(level_input, out_grad, conv_weight, norm_gain, norm_shift):
    grp = jnp.kron(jnp.eye(G, dtype=F32), jnp.ones((10, 10), F32))
    vm = pl.BlockSpec(memory_space=pltpu.VMEM)
    dma = pltpu.SemaphoreType.DMA
    V = pltpu.VMEM
    up, dw, par = pl.pallas_call(
        kernel,
        out_shape=(
            jax.ShapeDtypeStruct((512, 320), BF16),
            jax.ShapeDtypeStruct((135, 320), F32),
            jax.ShapeDtypeStruct((3, 320), F32),
        ),
        in_specs=[vm, vm, pl.BlockSpec(memory_space=pl.ANY), vm, vm, vm],
        out_specs=(vm, vm, vm),
        scratch_shapes=[
            V((27, 320, 320), BF16), V((3, 6, 160, 320), BF16), V((3, 6, 160, 320), BF16),
            V((4, 3, 160, 128), F32), V((2, 160, 128), F32),
            V((2, 4, 3, 16, 128), F32), V((4, 3, 16, 128), F32), V((4, 3, 16, 128), F32),
            V((8, 320), F32), V((8, 8, 320), F32), V((8, 320), F32), V((8, 8, 320), F32),
            V((8, 320), F32), V((8, 8, 320), F32), V((8, 320), F32), V((8, 8, 320), F32),
            V((512, 320), BF16), V((512, 320), BF16), V((320, 1024), BF16),
            V((512, 320), F32), V((512, 320), F32), V((8, 320), F32), V((14 * 320, 320), F32),
            V((4, SUB, ROWS, 320), BF16), V((4, SUB, ROWS, 320), BF16), V((4, SUB, ROWS, 320), BF16),
            V((8, 136, 320), F32), V((4, 136, 320), F32),
            V((512, 320), BF16), V((512, 320), BF16),
            dma(()), dma((2,)), dma((2,)), dma((2,)), dma((2,)), dma(()), dma(()), dma(()), dma(()),
            dma((8,)), dma((8,)), dma((8,)), dma((8,)), dma((8,)), dma((8,)), dma((8,)), dma((8,)),
            dma((4, SUB)), dma((4, SUB)), dma((4, SUB)), dma((8,)), dma((4,)), dma(()), dma(()),
        ],
        compiler_params=pltpu.CompilerParams(
            collective_id=0, has_side_effects=True, vmem_limit_bytes=60 * 1024 * 1024
        ),
    )(
        level_input.reshape(512, 320), out_grad.reshape(4, 128, 320), conv_weight.reshape(27, 320, 320),
        norm_gain, norm_shift, grp,
    )
    return up.reshape(1, 4, 8, 16, 320), dw[None], par[None]


def solution(mesh):
    return jax.shard_map(
        local,
        mesh=mesh,
        in_specs=(
            P("section", None, "gy", "gx", None),
            P("section", None, "gy", "gx", None),
            P("section", None, None, None),
            P("section", None),
            P("section", None),
        ),
        out_specs=(
            P("section", None, "gy", "gx", None),
            P("section", ("gy", "gx"), None),
            P("section", None, None),
        ),
        check_vma=False,
    )
```

```python
import jax
import jax.numpy as jnp
from jax import lax
from jax.experimental import pallas as pl
from jax.experimental.pallas import tpu as pltpu
from jax.sharding import PartitionSpec as P

G = 32
EPS = 1e-05
MESH = pl.DeviceIdType.MESH
SLAB = 1080
F32 = jnp.float32
BF16 = jnp.bfloat16


def pack(u):
    rem = u[:, 256:320]
    wide = jnp.concatenate([rem[0:72], jnp.concatenate([rem[72:136], jnp.zeros((8, 64), F32)], axis=0)], axis=1)
    low = jnp.concatenate([wide[40:72], jnp.zeros((8, 128), F32)], axis=0)
    return u[:, 0:256], jnp.concatenate([wide[0:40], low], axis=1)


def unpack(t):
    q = t[136:176]
    wide = jnp.concatenate([q[:, 0:128], q[0:32, 128:256]], axis=0)
    rem = jnp.concatenate([wide[:, 0:64], wide[0:64, 64:128]], axis=0)
    return jnp.concatenate([t[0:136], rem], axis=1)[0:135]


def kernel(x_ref, g_ref, w_hbm, gain_ref, shift_ref,
           up_ref, dw_ref, par_ref,
           wbuf, gs, pgs, gf, tmp, edge_out, edge_l, edge_r,
           st_x, rx_sx, st_z, rx_sz, pa_x, rx_px, pa_z, rx_pz,
           unit_own, unit_par, unit_t, acc, normed_b, slope_b, part, own,
           sbuf, ra, rb, bown, bs, bra, brb, xs, xm, xr, fsend, frecv, bfin, brecv, lsend, lrecv,
           wsem, zsem, zrsem, esem, ersem, gsem, grsem, usem, ursem,
           sxs, sxr, szs, szr, pxs, pxr, pzs, pzr,
           ssem, rasem, rbsem, bssem, brasem, brbsem, xssem, xmsem, xrsem,
           fsem, frsem, bfsem, bfrsem, ysem, yrsem):
    s = lax.axis_index("section")
    z = lax.axis_index("gy")
    me = lax.axis_index("gx")
    core = me % 2
    xc = me // 2
    partner = xc * 2 + 1 - core

    wcopy = pltpu.make_async_copy(w_hbm, wbuf, wsem)
    wcopy.start()

    barrier = pltpu.get_barrier_semaphore()
    for d in range(1, 8):
        pl.semaphore_signal(barrier, inc=1, device_id={"gx": (me + d) % 8}, device_id_type=MESH)
        pl.semaphore_signal(barrier, inc=1, device_id={"gy": (z + d) % 8}, device_id_type=MESH)

    @pl.when(s > 0)
    def _():
        pl.semaphore_signal(barrier, inc=1, device_id={"section": s - 1}, device_id_type=MESH)

    @pl.when(s < 3)
    def _():
        pl.semaphore_signal(barrier, inc=1, device_id={"section": s + 1}, device_id_type=MESH)

    def stat_body(i, carry):
        a, b = carry
        v = x_ref[pl.ds(pl.multiple_of(i * 64, 64), 64), :].astype(F32)
        return a + jnp.sum(v.reshape(8, 8, 320), axis=0), b + jnp.sum((v * v).reshape(8, 8, 320), axis=0)

    zero8 = jnp.zeros((8, 320), F32)
    a, b = lax.fori_loop(0, 8, stat_body, (zero8, zero8))
    st_x[...] = zero8
    st_x[0:1, :] = jnp.sum(a, axis=0, keepdims=True)
    st_x[1:2, :] = jnp.sum(b, axis=0, keepdims=True)

    first_entry = 14 + jnp.where(s > 0, 1, 0) + jnp.where(s < 3, 1, 0)
    pl.semaphore_wait(barrier, first_entry)

    def gather(src, dst, ssems, rsems, axis, at):
        out = []
        for d in range(1, 8):
            to = (at + d) % 8
            out.append(pltpu.make_async_remote_copy(
                src_ref=src, dst_ref=dst.at[at], send_sem=ssems.at[d], recv_sem=rsems.at[at],
                device_id={axis: to}, device_id_type=MESH))
            out[-1].start()
        dst[pl.ds(at, 1)] = src[...][None]

    def gathered(src, dst, ssems, rsems, axis, at):
        for d in range(1, 8):
            frm = (at + d) % 8
            cp = pltpu.make_async_remote_copy(
                src_ref=src, dst_ref=dst.at[frm], send_sem=ssems.at[d], recv_sem=rsems.at[frm],
                device_id={axis: frm}, device_id_type=MESH)
            cp.wait_send()
            cp.wait_recv()
        tot = dst[0]
        for d in range(1, 8):
            tot = tot + dst[d]
        return tot

    def halo(src_row, dst_row, to, i):
        return pltpu.make_async_remote_copy(
            src_ref=g_ref.at[:, pl.ds(src_row, 16), :],
            dst_ref=gs.at[1, pl.ds(1, 4), pl.ds(dst_row, 16), :],
            send_sem=zsem.at[i], recv_sem=zrsem.at[i], device_id={"gy": to}, device_id_type=MESH)

    up_halo = halo(0, 144, jnp.maximum(z - 1, 0), 0)
    down_halo = halo(112, 0, jnp.minimum(z + 1, 7), 1)
    pl.when(z > 0)(lambda: up_halo.start())
    pl.when(z < 7)(lambda: down_halo.start())
    gather(st_x, rx_sx, sxs, sxr, "gx", me)

    zrow = jnp.zeros((4, 16, 320), BF16)
    part[14 * 320:14 * 320 + 8, :] = zero8
    for c in range(3):
        pgs[c, 0] = jnp.zeros((160, 320), BF16)
        pgs[c, 5] = jnp.zeros((160, 320), BF16)
        gs[c, 0] = jnp.zeros((160, 320), BF16)
        gs[c, 5] = jnp.zeros((160, 320), BF16)

    @pl.when(z == 0)
    def _():
        gs[1, 1:5, 0:16, :] = zrow

    @pl.when(z == 7)
    def _():
        gs[1, 1:5, 144:160, :] = zrow

    bsum = jnp.zeros((1, 320), F32)
    for f in range(4):
        v = g_ref[f]
        gs[1, 1 + f, 16:144, :] = v
        v = v.astype(F32)
        bsum = bsum + jnp.sum(v, axis=0, keepdims=True)
    pa_x[...] = zero8
    pa_x[2:3, :] = bsum

    @pl.when(z > 0)
    def _():
        up_halo.wait_send()
        down_halo.wait_recv()

    @pl.when(z < 7)
    def _():
        down_halo.wait_send()
        up_halo.wait_recv()

    for f in range(4):
        v = gs[1, 1 + f].astype(F32)
        gf[f, 0] = v[:, 0:128]
        gf[f, 1] = v[:, 128:256]
        gf[f, 2] = jnp.concatenate([v[:, 256:320], jnp.zeros((160, 64), F32)], axis=1)
    for f in range(4):
        for l in range(3):
            edge_out[0, f, l] = jnp.zeros((16, 128), F32)
            edge_out[1, f, l] = jnp.zeros((16, 128), F32)
            edge_out[0, f, l, 0:10, :] = gf[f, l, pl.ds(0, 10, stride=16), :]
            edge_out[1, f, l, 0:10, :] = gf[f, l, pl.ds(15, 10, stride=16), :]
    to_left = pltpu.make_async_remote_copy(
        src_ref=edge_out.at[0], dst_ref=edge_r, send_sem=esem.at[0], recv_sem=ersem.at[0],
        device_id={"gx": jnp.maximum(me - 1, 0)}, device_id_type=MESH)
    to_right = pltpu.make_async_remote_copy(
        src_ref=edge_out.at[1], dst_ref=edge_l, send_sem=esem.at[1], recv_sem=ersem.at[1],
        device_id={"gx": jnp.minimum(me + 1, 7)}, device_id_type=MESH)
    pl.when(me > 0)(lambda: to_left.start())
    pl.when(me < 7)(lambda: to_right.start())

    @pl.when(me == 0)
    def _():
        edge_l[...] = jnp.zeros((4, 3, 16, 128), F32)

    @pl.when(me == 7)
    def _():
        edge_r[...] = jnp.zeros((4, 3, 16, 128), F32)

    st_z[...] = gathered(st_x, rx_sx, sxs, sxr, "gx", me)
    gather(st_z, rx_sz, szs, szr, "gy", z)

    @pl.when(me > 0)
    def _():
        to_left.wait_send()
        to_right.wait_recv()

    @pl.when(me < 7)
    def _():
        to_right.wait_send()
        to_left.wait_recv()

    for f in range(4):
        for l in range(3):
            w = 128 if l < 2 else 64
            v = gf[f, l]
            tmp[0] = pltpu.roll(v, 1, 0)
            tmp[1] = pltpu.roll(v, 159, 0)
            tmp[0, pl.ds(0, 10, stride=16), :] = edge_l[f, l, 0:10, :]
            tmp[1, pl.ds(15, 10, stride=16), :] = edge_r[f, l, 0:10, :]
            gs[2, 1 + f, :, 128 * l:128 * l + w] = tmp[0, :, 0:w].astype(BF16)
            gs[0, 1 + f, :, 128 * l:128 * l + w] = tmp[1, :, 0:w].astype(BF16)
    swap = pltpu.make_async_remote_copy(
        src_ref=gs.at[:, pl.ds(1, 4)], dst_ref=pgs.at[:, pl.ds(1, 4)], send_sem=gsem, recv_sem=grsem,
        device_id={"gx": partner}, device_id_type=MESH)
    swap.start()

    def window(ref, c, a, b):
        v = ref[c, pl.ds(2 - a, 4), pl.ds(pl.multiple_of((2 - b) * 16, 16), 128), :]
        return v.reshape(512, 320)

    ia = jnp.floor((lax.broadcasted_iota(jnp.int32, (320, 320), 0).astype(F32) + 0.5) * 0.1)
    ib = jnp.floor((lax.broadcasted_iota(jnp.int32, (320, 320), 1).astype(F32) + 0.5) * 0.1)
    grp = jnp.where(ia == ib, 1.0, 0.0).astype(F32)
    members = float(512 * 64 * 10)
    tot = gathered(st_z, rx_sz, szs, szr, "gy", z)
    per = jnp.dot(tot, grp, precision=lax.Precision.HIGHEST, preferred_element_type=F32) / members
    mean = per[0:1, :]
    var = per[1:2, :] - mean * mean
    inv = 1.0 / jnp.sqrt(var + EPS)
    gain = gain_ref[...]
    shift = shift_ref[...]

    def act_body(i, carry):
        rows = pl.ds(pl.multiple_of(i * 64, 64), 64)
        n = (x_ref[rows, :].astype(F32) - mean) * inv
        y = n * gain + shift
        sg = jax.nn.sigmoid(y)
        unit_own[rows, :] = (y * sg).astype(BF16)
        slope_b[rows, :] = sg * (1.0 + y * (1.0 - sg))
        normed_b[rows, :] = n
        return carry

    lax.fori_loop(0, 8, act_body, 0)
    swap_u = pltpu.make_async_remote_copy(
        src_ref=unit_own, dst_ref=unit_par, send_sem=usem, recv_sem=ursem,
        device_id={"gx": partner}, device_id_type=MESH)
    swap_u.start()
    unit_t[:, 0:512] = unit_own[...].T
    swap.wait()
    swap_u.wait()
    unit_t[:, 512:1024] = unit_par[...].T

    def taps(t, carry):
        k = 13 * core + t
        ab = k // 3
        c = k % 3
        a, b = ab // 3, ab % 3
        win = jnp.concatenate([window(gs, c, a, b), window(pgs, c, a, b)], axis=0)
        part[pl.ds(pl.multiple_of(t * 320, 64), 320), :] = jnp.dot(unit_t[...], win, preferred_element_type=F32)
        return carry

    lax.fori_loop(0, 14, taps, 0)

    def packing(j, carry):
        for d in range(8):
            lo = (135 * d) // 8 * 8
            v = part[pl.ds(pl.multiple_of(160 * core + SLAB * j + lo, 8), 144), :]
            main, rest = pack(v[135 * d - lo:135 * d - lo + 136, :])
            own[j, d, 0:136, :] = main
            own[j, d, 136:176, :] = rest
        return carry

    lax.fori_loop(0, 4, packing, 0)

    def relay(j, tau, top, mine, sb, up_in, down_in, s_send, s_up, s_down, result):
        delta = (4 * core + j - z + 8) % 8
        going_up = (delta >= 1) & (delta <= top)
        going_down = delta > top

        def sends_up():
            return pltpu.make_async_remote_copy(
                src_ref=sb, dst_ref=up_in, send_sem=s_send, recv_sem=s_up,
                device_id={"gy": (z + 1) % 8}, device_id_type=MESH)

        def sends_down():
            return pltpu.make_async_remote_copy(
                src_ref=sb, dst_ref=down_in, send_sem=s_send, recv_sem=s_down,
                device_id={"gy": (z + 7) % 8}, device_id_type=MESH)

        for cond, when, send, got in (
            (going_up, top - delta, sends_up, up_in),
            (going_down, delta - top - 1, sends_down, down_in),
        ):
            @pl.when(cond & (when == tau))
            def _(send=send, got=got):
                if tau == 0:
                    sb[...] = mine[...].astype(sb.dtype)
                else:
                    send().wait_recv()
                    sb[...] = (mine[...] + got[...].astype(F32)).astype(sb.dtype)
                send().start()

        if tau == 4:
            @pl.when(delta == 0)
            def _():
                sends_up().wait_recv()
                sends_down().wait_recv()
                result[...] = mine[...] + up_in[...].astype(F32) + down_in[...].astype(F32)

    def chain_a(tau):
        def one(j, carry):
            for i in range(4):
                relay(j, tau, 4 - i % 2, own.at[j, 2 * i], sbuf.at[j, i], ra.at[j, i], rb.at[j, i],
                      ssem.at[j, i], rasem.at[j, i], rbsem.at[j, i], fsend.at[i])
            return carry

        lax.fori_loop(0, 4, one, 0)

    def chain_b(tau):
        for j in range(4):
            relay(j, tau, 4 - j % 2, bown.at[j], bs.at[j], bra.at[j], brb.at[j],
                  bssem.at[j], brasem.at[j], brbsem.at[j], bfin)

    def ring(j, e, dst, rsem):
        plus = e == 1 or (e == 2 and j % 2 == 0)
        to = ((xc + (1 if plus else 3)) % 4) * 2 + core
        return pltpu.make_async_remote_copy(
            src_ref=xs.at[j, e - 1], dst_ref=dst, send_sem=xssem.at[j, e - 1], recv_sem=rsem,
            device_id={"gx": to}, device_id_type=MESH)

    def odd(j, e):
        return own[j, 2 * ((xc + e) % 4) + 1]

    def long_in(j):
        return ring(j, 2, xm.at[j], xmsem.at[j])

    def root_in(j, e):
        return ring(j, e, xr.at[j, e // 2], xrsem.at[j, e // 2])

    def ring_0():
        for j in range(4):
            xs[j, 1] = odd(j, 2).astype(BF16)
            long_in(j).start()
        for j in range(4):
            e = 3 if j % 2 == 0 else 1
            xs[j, e - 1] = odd(j, e).astype(BF16)
            root_in(j, e).start()

    def ring_1():
        for j in range(4):
            e = 1 if j % 2 == 0 else 3
            long_in(j).wait_recv()
            xs[j, e - 1] = (odd(j, e) + xm[j].astype(F32)).astype(BF16)
            root_in(j, e).start()

    def ring_2():
        for j in range(4):
            root_in(j, 1).wait_recv()
            root_in(j, 3).wait_recv()
            bown[j] = odd(j, 0) + xr[j, 0].astype(F32) + xr[j, 1].astype(F32)

    chain_a(0)
    ring_0()

    wcopy.wait()

    def side(ab, carry):
        a, b = ab // 3, ab % 3
        tot = None
        for c in range(3):
            wk = wbuf[ab * 3 + c]
            d = lax.dot_general(window(gs, c, a, b), wk, (((1,), (1,)), ((), ())), preferred_element_type=F32)
            tot = d if tot is None else tot + d
        acc[...] += tot
        return carry

    acc[...] = jnp.zeros((512, 320), F32)
    lax.fori_loop(0, 9, side, 0)

    def grad_body(i, carry):
        p0, p1 = carry
        rows = pl.ds(pl.multiple_of(i * 64, 64), 64)
        ag = acc[rows, :] * slope_b[rows, :]
        acc[rows, :] = ag
        return (p0 + jnp.sum((ag * normed_b[rows, :]).reshape(8, 8, 320), axis=0),
                p1 + jnp.sum(ag.reshape(8, 8, 320), axis=0))

    p0, p1 = lax.fori_loop(0, 8, grad_body, (zero8, zero8))
    pa_x[0:1, :] = jnp.sum(p0, axis=0, keepdims=True)
    pa_x[1:2, :] = jnp.sum(p1, axis=0, keepdims=True)
    gather(pa_x, rx_px, pxs, pxr, "gx", me)

    ring_1()
    chain_a(1)
    pa_z[...] = gathered(pa_x, rx_px, pxs, pxr, "gx", me)
    gather(pa_z, rx_pz, pzs, pzr, "gy", z)
    ring_2()
    chain_b(0)
    chain_a(2)

    ptot = gathered(pa_z, rx_pz, pzs, pzr, "gy", z)
    par_ref[...] = ptot[0:3, :]
    gg = jnp.dot(ptot * gain, grp, precision=lax.Precision.HIGHEST, preferred_element_type=F32) / members
    second = gg[0:1, :]
    first = gg[1:2, :]

    def lev(i, carry):
        rows = pl.ds(pl.multiple_of(i * 64, 64), 64)
        gv = g_ref[i // 2, pl.ds(pl.multiple_of((i % 2) * 64, 64), 64), :].astype(F32)
        ng = (acc[rows, :] * gain - first - normed_b[rows, :] * second) * inv
        lsend[rows, :] = (gv + ng).astype(BF16)
        return carry

    lax.fori_loop(0, 8, lev, 0)
    ycopy = pltpu.make_async_remote_copy(
        src_ref=lsend, dst_ref=lrecv, send_sem=ysem, recv_sem=yrsem,
        device_id={"section": jnp.maximum(s - 1, 0)}, device_id_type=MESH)
    pl.when(s > 0)(lambda: ycopy.start())

    chain_b(1)
    chain_a(3)
    chain_b(2)
    chain_a(4)

    root = z // 4

    def to_even(x2):
        return pltpu.make_async_remote_copy(
            src_ref=fsend.at[x2], dst_ref=frecv.at[xc], send_sem=fsem.at[x2], recv_sem=frsem.at[xc],
            device_id={"gx": 2 * x2}, device_id_type=MESH)

    def to_odd():
        return pltpu.make_async_remote_copy(
            src_ref=bfin, dst_ref=brecv, send_sem=bfsem, recv_sem=bfrsem,
            device_id={"gx": partner}, device_id_type=MESH)

    for i in range(4):
        x2 = (xc + i) % 4
        if i:
            pl.when(core == root)(lambda x2=x2: to_even(x2).start())
        else:
            pl.when((core == root) & (core == 1))(lambda x2=x2: to_even(x2).start())

            @pl.when((core == root) & (core == 0))
            def _():
                frecv[pl.ds(xc, 1)] = fsend[pl.ds(xc, 1)]

    chain_b(3)
    chain_b(4)

    @pl.when((root == 0) & (core == 0))
    def _():
        to_odd().start()

    @pl.when((root == 1) & (core == 1))
    def _():
        dw_ref[...] = unpack(bfin[...])

    @pl.when((root == 0) & (core == 1))
    def _():
        to_odd().wait_recv()
        dw_ref[...] = unpack(brecv[...])

    @pl.when(core == 0)
    def _():
        for q in range(4):
            @pl.when((root == 1) | (xc != q))
            def _(q=q):
                pltpu.make_async_remote_copy(
                    src_ref=fsend.at[q], dst_ref=frecv.at[q], send_sem=fsem.at[q], recv_sem=frsem.at[q],
                    device_id={"gx": partner}, device_id_type=MESH).wait_recv()

        dw_ref[...] = unpack((frecv[0] + frecv[1]) + (frecv[2] + frecv[3]))

    for i in range(4):
        x2 = (xc + i) % 4
        if i:
            pl.when(core == root)(lambda x2=x2: to_even(x2).wait_send())
        else:
            pl.when((core == root) & (core == 1))(lambda x2=x2: to_even(x2).wait_send())

    @pl.when((root == 0) & (core == 0))
    def _():
        to_odd().wait_send()

    def drain(j, carry):
        @pl.when((4 * core + j - z + 8) % 8 != 0)
        def _():
            for i in range(4):
                pltpu.make_async_remote_copy(
                    src_ref=sbuf.at[j, i], dst_ref=ra.at[j, i], send_sem=ssem.at[j, i],
                    recv_sem=rasem.at[j, i], device_id={"gy": (z + 1) % 8}, device_id_type=MESH).wait_send()
            pltpu.make_async_remote_copy(
                src_ref=bs.at[j], dst_ref=bra.at[j], send_sem=bssem.at[j],
                recv_sem=brasem.at[j], device_id={"gy": (z + 1) % 8}, device_id_type=MESH).wait_send()

        return carry

    lax.fori_loop(0, 4, drain, 0)
    for j in range(4):
        long_in(j).wait_send()
        root_in(j, 1).wait_send()
        root_in(j, 3).wait_send()
    pl.when(s > 0)(lambda: ycopy.wait_send())

    @pl.when(s < 3)
    def _():
        ycopy.wait_recv()
        up_ref[...] = lrecv[...]

    @pl.when(s == 3)
    def _():
        up_ref[...] = jnp.zeros((512, 320), BF16)


def local(level_input, out_grad, conv_weight, norm_gain, norm_shift):
    vm = pl.BlockSpec(memory_space=pltpu.VMEM)
    dma = pltpu.SemaphoreType.DMA
    V = pltpu.VMEM
    up, dw, par = pl.pallas_call(
        kernel,
        out_shape=(
            jax.ShapeDtypeStruct((512, 320), BF16),
            jax.ShapeDtypeStruct((135, 320), F32),
            jax.ShapeDtypeStruct((3, 320), F32),
        ),
        in_specs=[vm, vm, pl.BlockSpec(memory_space=pl.ANY), vm, vm],
        out_specs=(vm, vm, vm),
        scratch_shapes=[
            V((27, 320, 320), BF16), V((3, 6, 160, 320), BF16), V((3, 6, 160, 320), BF16),
            V((4, 3, 160, 128), F32), V((2, 160, 128), F32),
            V((2, 4, 3, 16, 128), F32), V((4, 3, 16, 128), F32), V((4, 3, 16, 128), F32),
            V((8, 320), F32), V((8, 8, 320), F32), V((8, 320), F32), V((8, 8, 320), F32),
            V((8, 320), F32), V((8, 8, 320), F32), V((8, 320), F32), V((8, 8, 320), F32),
            V((512, 320), BF16), V((512, 320), BF16), V((320, 1024), BF16),
            V((512, 320), F32), V((512, 320), F32), V((512, 320), F32), V((14 * 320 + 8, 320), F32), V((4, 8, 176, 256), F32),
            V((4, 4, 176, 256), BF16), V((4, 4, 176, 256), BF16), V((4, 4, 176, 256), BF16),
            V((4, 176, 256), F32), V((4, 176, 256), F32), V((4, 176, 256), F32), V((4, 176, 256), F32),
            V((4, 3, 176, 256), BF16), V((4, 176, 256), BF16), V((4, 2, 176, 256), BF16),
            V((4, 176, 256), F32), V((4, 176, 256), F32), V((176, 256), F32), V((176, 256), F32),
            V((512, 320), BF16), V((512, 320), BF16),
            dma(()), dma((2,)), dma((2,)), dma((2,)), dma((2,)), dma(()), dma(()), dma(()), dma(()),
            dma((8,)), dma((8,)), dma((8,)), dma((8,)), dma((8,)), dma((8,)), dma((8,)), dma((8,)),
            dma((4, 4)), dma((4, 4)), dma((4, 4)), dma((4,)), dma((4,)), dma((4,)), dma((4, 3)), dma((4,)), dma((4, 2)),
            dma((4,)), dma((4,)), dma(()), dma(()), dma(()), dma(()),
        ],
        compiler_params=pltpu.CompilerParams(
            collective_id=0, has_side_effects=True, vmem_limit_bytes=60 * 1024 * 1024
        ),
    )(
        level_input.reshape(512, 320), out_grad.reshape(4, 128, 320), conv_weight.reshape(27, 320, 320),
        norm_gain, norm_shift,
    )
    return up.reshape(1, 4, 8, 16, 320), dw[None], par[None]


def solution(mesh):
    return jax.shard_map(
        local,
        mesh=mesh,
        in_specs=(
            P("section", None, "gy", "gx", None),
            P("section", None, "gy", "gx", None),
            P("section", None, None, None),
            P("section", None),
            P("section", None),
        ),
        out_specs=(
            P("section", None, "gy", "gx", None),
            P("section", ("gy", "gx"), None),
            P("section", None, None),
        ),
        check_vma=False,
    )
```

```python
import jax
import jax.numpy as jnp
from jax import lax
from jax.experimental import pallas as pl
from jax.experimental.pallas import tpu as pltpu
from jax.sharding import PartitionSpec as P

G = 32
EPS = 1e-05
MESH = pl.DeviceIdType.MESH
SLAB = 1080
F32 = jnp.float32
BF16 = jnp.bfloat16


def pack(u):
    rem = u[:, 256:320]
    wide = jnp.concatenate([rem[0:72], jnp.concatenate([rem[72:136], jnp.zeros((8, 64), F32)], axis=0)], axis=1)
    low = jnp.concatenate([wide[40:72], jnp.zeros((8, 128), F32)], axis=0)
    return u[:, 0:256], jnp.concatenate([wide[0:40], low], axis=1)


def unpack(t):
    q = t[136:176]
    wide = jnp.concatenate([q[:, 0:128], q[0:32, 128:256]], axis=0)
    rem = jnp.concatenate([wide[:, 0:64], wide[0:64, 64:128]], axis=0)
    return jnp.concatenate([t[0:136], rem], axis=1)[0:135]


def kernel(x_ref, g_ref, w_hbm, gain_ref, shift_ref,
           up_ref, dw_ref, par_ref,
           wbuf, gs, pgs, gf, tmp, edge_out, edge_l, edge_r,
           st_x, rx_sx, st_z, rx_sz, pa_x, rx_px, pa_z, rx_pz,
           unit_own, unit_par, unit_t, acc, normed_b, slope_b, part, own,
           sbuf, ra, rb, bown, bs, bra, xs, xm, xr, fsend, frecv, bfin, brecv, lsend, lrecv,
           wsem, zsem, zrsem, esem, ersem, gsem, grsem, usem, ursem,
           sxs, sxr, szs, szr, pxs, pxr, pzs, pzr,
           ssem, rasem, rbsem, bssem, brasem, xssem, xmsem, xrsem,
           fsem, frsem, bfsem, bfrsem, ysem, yrsem):
    s = lax.axis_index("section")
    z = lax.axis_index("gy")
    me = lax.axis_index("gx")
    core = me % 2
    xc = me // 2
    partner = xc * 2 + 1 - core

    wcopy = pltpu.make_async_copy(w_hbm, wbuf, wsem)
    wcopy.start()

    barrier = pltpu.get_barrier_semaphore()
    for d in range(1, 8):
        pl.semaphore_signal(barrier, inc=1, device_id={"gx": (me + d) % 8}, device_id_type=MESH)
        pl.semaphore_signal(barrier, inc=1, device_id={"gy": (z + d) % 8}, device_id_type=MESH)

    @pl.when(s > 0)
    def _():
        pl.semaphore_signal(barrier, inc=1, device_id={"section": s - 1}, device_id_type=MESH)

    @pl.when(s < 3)
    def _():
        pl.semaphore_signal(barrier, inc=1, device_id={"section": s + 1}, device_id_type=MESH)

    def stat_body(i, carry):
        a, b = carry
        v = x_ref[pl.ds(pl.multiple_of(i * 64, 64), 64), :].astype(F32)
        return a + jnp.sum(v.reshape(8, 8, 320), axis=0), b + jnp.sum((v * v).reshape(8, 8, 320), axis=0)

    zero8 = jnp.zeros((8, 320), F32)
    a, b = lax.fori_loop(0, 8, stat_body, (zero8, zero8))
    st_x[...] = zero8
    st_x[0:1, :] = jnp.sum(a, axis=0, keepdims=True)
    st_x[1:2, :] = jnp.sum(b, axis=0, keepdims=True)

    first_entry = 14 + jnp.where(s > 0, 1, 0) + jnp.where(s < 3, 1, 0)
    pl.semaphore_wait(barrier, first_entry)

    def gather(src, dst, ssems, rsems, axis, at):
        out = []
        for d in range(1, 8):
            to = (at + d) % 8
            out.append(pltpu.make_async_remote_copy(
                src_ref=src, dst_ref=dst.at[at], send_sem=ssems.at[d], recv_sem=rsems.at[at],
                device_id={axis: to}, device_id_type=MESH))
            out[-1].start()
        dst[pl.ds(at, 1)] = src[...][None]

    def gathered(src, dst, ssems, rsems, axis, at):
        for d in range(1, 8):
            frm = (at + d) % 8
            cp = pltpu.make_async_remote_copy(
                src_ref=src, dst_ref=dst.at[frm], send_sem=ssems.at[d], recv_sem=rsems.at[frm],
                device_id={axis: frm}, device_id_type=MESH)
            cp.wait_send()
            cp.wait_recv()
        tot = dst[0]
        for d in range(1, 8):
            tot = tot + dst[d]
        return tot

    def halo(src_row, dst_row, to, i):
        return pltpu.make_async_remote_copy(
            src_ref=g_ref.at[:, pl.ds(src_row, 16), :],
            dst_ref=gs.at[1, pl.ds(1, 4), pl.ds(dst_row, 16), :],
            send_sem=zsem.at[i], recv_sem=zrsem.at[i], device_id={"gy": to}, device_id_type=MESH)

    up_halo = halo(0, 144, jnp.maximum(z - 1, 0), 0)
    down_halo = halo(112, 0, jnp.minimum(z + 1, 7), 1)
    pl.when(z > 0)(lambda: up_halo.start())
    pl.when(z < 7)(lambda: down_halo.start())
    gather(st_x, rx_sx, sxs, sxr, "gx", me)

    zrow = jnp.zeros((4, 16, 320), BF16)
    part[14 * 320:14 * 320 + 8, :] = zero8
    for c in range(3):
        pgs[c, 0] = jnp.zeros((160, 320), BF16)
        pgs[c, 5] = jnp.zeros((160, 320), BF16)
        gs[c, 0] = jnp.zeros((160, 320), BF16)
        gs[c, 5] = jnp.zeros((160, 320), BF16)

    @pl.when(z == 0)
    def _():
        gs[1, 1:5, 0:16, :] = zrow

    @pl.when(z == 7)
    def _():
        gs[1, 1:5, 144:160, :] = zrow

    bsum = jnp.zeros((1, 320), F32)
    for f in range(4):
        v = g_ref[f]
        gs[1, 1 + f, 16:144, :] = v
        v = v.astype(F32)
        bsum = bsum + jnp.sum(v, axis=0, keepdims=True)
    pa_x[...] = zero8
    pa_x[2:3, :] = bsum

    @pl.when(z > 0)
    def _():
        up_halo.wait_send()
        down_halo.wait_recv()

    @pl.when(z < 7)
    def _():
        down_halo.wait_send()
        up_halo.wait_recv()

    for f in range(4):
        v = gs[1, 1 + f].astype(F32)
        gf[f, 0] = v[:, 0:128]
        gf[f, 1] = v[:, 128:256]
        gf[f, 2] = jnp.concatenate([v[:, 256:320], jnp.zeros((160, 64), F32)], axis=1)
    for f in range(4):
        for l in range(3):
            edge_out[0, f, l] = jnp.zeros((16, 128), F32)
            edge_out[1, f, l] = jnp.zeros((16, 128), F32)
            edge_out[0, f, l, 0:10, :] = gf[f, l, pl.ds(0, 10, stride=16), :]
            edge_out[1, f, l, 0:10, :] = gf[f, l, pl.ds(15, 10, stride=16), :]
    to_left = pltpu.make_async_remote_copy(
        src_ref=edge_out.at[0], dst_ref=edge_r, send_sem=esem.at[0], recv_sem=ersem.at[0],
        device_id={"gx": jnp.maximum(me - 1, 0)}, device_id_type=MESH)
    to_right = pltpu.make_async_remote_copy(
        src_ref=edge_out.at[1], dst_ref=edge_l, send_sem=esem.at[1], recv_sem=ersem.at[1],
        device_id={"gx": jnp.minimum(me + 1, 7)}, device_id_type=MESH)
    pl.when(me > 0)(lambda: to_left.start())
    pl.when(me < 7)(lambda: to_right.start())

    @pl.when(me == 0)
    def _():
        edge_l[...] = jnp.zeros((4, 3, 16, 128), F32)

    @pl.when(me == 7)
    def _():
        edge_r[...] = jnp.zeros((4, 3, 16, 128), F32)

    st_z[...] = gathered(st_x, rx_sx, sxs, sxr, "gx", me)
    gather(st_z, rx_sz, szs, szr, "gy", z)

    @pl.when(me > 0)
    def _():
        to_left.wait_send()
        to_right.wait_recv()

    @pl.when(me < 7)
    def _():
        to_right.wait_send()
        to_left.wait_recv()

    for f in range(4):
        for l in range(3):
            w = 128 if l < 2 else 64
            v = gf[f, l]
            tmp[0] = pltpu.roll(v, 1, 0)
            tmp[1] = pltpu.roll(v, 159, 0)
            tmp[0, pl.ds(0, 10, stride=16), :] = edge_l[f, l, 0:10, :]
            tmp[1, pl.ds(15, 10, stride=16), :] = edge_r[f, l, 0:10, :]
            gs[2, 1 + f, :, 128 * l:128 * l + w] = tmp[0, :, 0:w].astype(BF16)
            gs[0, 1 + f, :, 128 * l:128 * l + w] = tmp[1, :, 0:w].astype(BF16)
    swap = pltpu.make_async_remote_copy(
        src_ref=gs.at[:, pl.ds(1, 4)], dst_ref=pgs.at[:, pl.ds(1, 4)], send_sem=gsem, recv_sem=grsem,
        device_id={"gx": partner}, device_id_type=MESH)
    swap.start()

    def window(ref, c, a, b):
        v = ref[c, pl.ds(2 - a, 4), pl.ds(pl.multiple_of((2 - b) * 16, 16), 128), :]
        return v.reshape(512, 320)

    ia = jnp.floor((lax.broadcasted_iota(jnp.int32, (320, 320), 0).astype(F32) + 0.5) * 0.1)
    ib = jnp.floor((lax.broadcasted_iota(jnp.int32, (320, 320), 1).astype(F32) + 0.5) * 0.1)
    grp = jnp.where(ia == ib, 1.0, 0.0).astype(F32)
    members = float(512 * 64 * 10)
    tot = gathered(st_z, rx_sz, szs, szr, "gy", z)
    per = jnp.dot(tot, grp, precision=lax.Precision.HIGHEST, preferred_element_type=F32) / members
    mean = per[0:1, :]
    var = per[1:2, :] - mean * mean
    inv = 1.0 / jnp.sqrt(var + EPS)
    gain = gain_ref[...]
    shift = shift_ref[...]

    def act_body(i, carry):
        rows = pl.ds(pl.multiple_of(i * 64, 64), 64)
        n = (x_ref[rows, :].astype(F32) - mean) * inv
        y = n * gain + shift
        sg = jax.nn.sigmoid(y)
        unit_own[rows, :] = (y * sg).astype(BF16)
        slope_b[rows, :] = sg * (1.0 + y * (1.0 - sg))
        normed_b[rows, :] = n
        return carry

    lax.fori_loop(0, 8, act_body, 0)
    swap_u = pltpu.make_async_remote_copy(
        src_ref=unit_own, dst_ref=unit_par, send_sem=usem, recv_sem=ursem,
        device_id={"gx": partner}, device_id_type=MESH)
    swap_u.start()
    unit_t[:, 0:512] = unit_own[...].T
    swap.wait()
    swap_u.wait()
    unit_t[:, 512:1024] = unit_par[...].T

    def taps(t, carry):
        k = 13 * core + t
        ab = k // 3
        c = k % 3
        b = ab % 3
        rows = pl.ds(pl.multiple_of((2 - b) * 16, 16), 128)
        out = pl.ds(pl.multiple_of(t * 320, 64), 320)
        for a in range(3):
            f0, n = max(0, a - 1), 4 - abs(a - 1)

            @pl.when(ab // 3 == a)
            def _(a=a, f0=f0, n=n):
                wins = [ref[c, pl.ds(f0 + 2 - a, n), rows, :].reshape(n * 128, 320) for ref in (gs, pgs)]
                units = [unit_t[:, 512 * i + 128 * f0:512 * i + 128 * (f0 + n)] for i in range(2)]
                part[out, :] = jnp.dot(
                    jnp.concatenate(units, axis=1), jnp.concatenate(wins, axis=0), preferred_element_type=F32)

        return carry

    lax.fori_loop(0, 14, taps, 0)

    def packing(j, carry):
        for d in range(8):
            lo = (135 * d) // 8 * 8
            v = part[pl.ds(pl.multiple_of(160 * core + SLAB * j + lo, 8), 144), :]
            main, rest = pack(v[135 * d - lo:135 * d - lo + 136, :])
            own[j, d, 0:136, :] = main
            own[j, d, 136:176, :] = rest
        return carry

    lax.fori_loop(0, 4, packing, 0)

    def relay(j, tau, top, mine, sb, up_in, down_in, s_send, s_up, s_down, result):
        delta = (4 * core + j - z + 8) % 8
        going_up = (delta >= 1) & (delta <= top)
        going_down = delta > top

        def sends_up():
            return pltpu.make_async_remote_copy(
                src_ref=sb, dst_ref=up_in, send_sem=s_send, recv_sem=s_up,
                device_id={"gy": (z + 1) % 8}, device_id_type=MESH)

        def sends_down():
            return pltpu.make_async_remote_copy(
                src_ref=sb, dst_ref=down_in, send_sem=s_send, recv_sem=s_down,
                device_id={"gy": (z + 7) % 8}, device_id_type=MESH)

        for cond, when, send, got in (
            (going_up, top - delta, sends_up, up_in),
            (going_down, delta - top - 1, sends_down, down_in),
        ):
            @pl.when(cond & (when == tau))
            def _(send=send, got=got):
                if tau == 0:
                    sb[...] = mine[...].astype(sb.dtype)
                else:
                    send().wait_recv()
                    sb[...] = (mine[...] + got[...].astype(F32)).astype(sb.dtype)
                send().start()

        if tau == 4:
            @pl.when(delta == 0)
            def _():
                sends_up().wait_recv()
                sends_down().wait_recv()
                result[...] = mine[...] + up_in[...].astype(F32) + down_in[...].astype(F32)

    def chain_a(tau):
        def one(j, carry):
            for i in range(4):
                relay(j, tau, 4 - i % 2, own.at[j, 2 * i], sbuf.at[j, i], ra.at[j, i], rb.at[j, i],
                      ssem.at[j, i], rasem.at[j, i], rbsem.at[j, i], fsend.at[i])
            return carry

        lax.fori_loop(0, 4, one, 0)

    def straight(j):
        return pltpu.make_async_remote_copy(
            src_ref=bs.at[j], dst_ref=bra.at[z], send_sem=bssem.at[j], recv_sem=brasem.at[z],
            device_id={"gy": 4 * core + j}, device_id_type=MESH)

    def straight_sends():
        for j in range(4):
            @pl.when(4 * core + j != z)
            def _(j=j):
                bs[j] = bown[j].astype(BF16)
                straight(j).start()

    def straight_sum():
        @pl.when(core == z // 4)
        def _():
            tot = bown[z - 4 * core]
            for d in range(1, 8):
                frm = (z + d) % 8
                pltpu.make_async_remote_copy(
                    src_ref=bs.at[0], dst_ref=bra.at[frm], send_sem=bssem.at[0], recv_sem=brasem.at[frm],
                    device_id={"gy": frm}, device_id_type=MESH).wait_recv()
                tot = tot + bra[frm].astype(F32)
            bfin[...] = tot

    def ring(j, e, dst, rsem):
        plus = e == 1 or (e == 2 and j % 2 == 0)
        to = ((xc + (1 if plus else 3)) % 4) * 2 + core
        return pltpu.make_async_remote_copy(
            src_ref=xs.at[j, e - 1], dst_ref=dst, send_sem=xssem.at[j, e - 1], recv_sem=rsem,
            device_id={"gx": to}, device_id_type=MESH)

    def odd(j, e):
        return own[j, 2 * ((xc + e) % 4) + 1]

    def long_in(j):
        return ring(j, 2, xm.at[j], xmsem.at[j])

    def root_in(j, e):
        return ring(j, e, xr.at[j, e // 2], xrsem.at[j, e // 2])

    def ring_0():
        for j in range(4):
            xs[j, 1] = odd(j, 2).astype(BF16)
            long_in(j).start()
        for j in range(4):
            e = 3 if j % 2 == 0 else 1
            xs[j, e - 1] = odd(j, e).astype(BF16)
            root_in(j, e).start()

    def ring_1():
        for j in range(4):
            e = 1 if j % 2 == 0 else 3
            long_in(j).wait_recv()
            xs[j, e - 1] = (odd(j, e) + xm[j].astype(F32)).astype(BF16)
            root_in(j, e).start()

    def ring_2():
        for j in range(4):
            root_in(j, 1).wait_recv()
            root_in(j, 3).wait_recv()
            bown[j] = odd(j, 0) + xr[j, 0].astype(F32) + xr[j, 1].astype(F32)

    ring_0()
    chain_a(0)

    wcopy.wait()

    def side(ab, carry):
        a, b = ab // 3, ab % 3
        tot = None
        for c in range(3):
            wk = wbuf[ab * 3 + c]
            d = lax.dot_general(window(gs, c, a, b), wk, (((1,), (1,)), ((), ())), preferred_element_type=F32)
            tot = d if tot is None else tot + d
        acc[...] += tot
        return carry

    acc[...] = jnp.zeros((512, 320), F32)
    lax.fori_loop(0, 4, side, 0)
    chain_a(1)
    lax.fori_loop(4, 7, side, 0)
    ring_1()
    lax.fori_loop(7, 9, side, 0)

    def grad_body(i, carry):
        p0, p1 = carry
        rows = pl.ds(pl.multiple_of(i * 64, 64), 64)
        ag = acc[rows, :] * slope_b[rows, :]
        acc[rows, :] = ag
        return (p0 + jnp.sum((ag * normed_b[rows, :]).reshape(8, 8, 320), axis=0),
                p1 + jnp.sum(ag.reshape(8, 8, 320), axis=0))

    p0, p1 = lax.fori_loop(0, 8, grad_body, (zero8, zero8))
    pa_x[0:1, :] = jnp.sum(p0, axis=0, keepdims=True)
    pa_x[1:2, :] = jnp.sum(p1, axis=0, keepdims=True)
    gather(pa_x, rx_px, pxs, pxr, "gx", me)

    chain_a(2)
    pa_z[...] = gathered(pa_x, rx_px, pxs, pxr, "gx", me)
    gather(pa_z, rx_pz, pzs, pzr, "gy", z)
    chain_a(3)
    ring_2()
    straight_sends()

    ptot = gathered(pa_z, rx_pz, pzs, pzr, "gy", z)
    par_ref[...] = ptot[0:3, :]
    gg = jnp.dot(ptot * gain, grp, precision=lax.Precision.HIGHEST, preferred_element_type=F32) / members
    second = gg[0:1, :]
    first = gg[1:2, :]

    def lev(i, carry):
        rows = pl.ds(pl.multiple_of(i * 64, 64), 64)
        gv = g_ref[i // 2, pl.ds(pl.multiple_of((i % 2) * 64, 64), 64), :].astype(F32)
        ng = (acc[rows, :] * gain - first - normed_b[rows, :] * second) * inv
        lsend[rows, :] = (gv + ng).astype(BF16)
        return carry

    lax.fori_loop(0, 8, lev, 0)
    ycopy = pltpu.make_async_remote_copy(
        src_ref=lsend, dst_ref=lrecv, send_sem=ysem, recv_sem=yrsem,
        device_id={"section": jnp.maximum(s - 1, 0)}, device_id_type=MESH)
    pl.when(s > 0)(lambda: ycopy.start())

    chain_a(4)

    root = z // 4

    def to_even(x2):
        return pltpu.make_async_remote_copy(
            src_ref=fsend.at[x2], dst_ref=frecv.at[xc], send_sem=fsem.at[x2], recv_sem=frsem.at[xc],
            device_id={"gx": 2 * x2}, device_id_type=MESH)

    def to_odd():
        return pltpu.make_async_remote_copy(
            src_ref=bfin, dst_ref=brecv, send_sem=bfsem, recv_sem=bfrsem,
            device_id={"gx": partner}, device_id_type=MESH)

    for i in range(4):
        x2 = (xc + i) % 4
        if i:
            pl.when(core == root)(lambda x2=x2: to_even(x2).start())
        else:
            pl.when((core == root) & (core == 1))(lambda x2=x2: to_even(x2).start())

            @pl.when((core == root) & (core == 0))
            def _():
                frecv[pl.ds(xc, 1)] = fsend[pl.ds(xc, 1)]

    straight_sum()

    @pl.when((root == 0) & (core == 0))
    def _():
        to_odd().start()

    @pl.when((root == 1) & (core == 1))
    def _():
        dw_ref[...] = unpack(bfin[...])

    @pl.when((root == 0) & (core == 1))
    def _():
        to_odd().wait_recv()
        dw_ref[...] = unpack(brecv[...])

    @pl.when(core == 0)
    def _():
        for q in range(4):
            @pl.when((root == 1) | (xc != q))
            def _(q=q):
                pltpu.make_async_remote_copy(
                    src_ref=fsend.at[q], dst_ref=frecv.at[q], send_sem=fsem.at[q], recv_sem=frsem.at[q],
                    device_id={"gx": partner}, device_id_type=MESH).wait_recv()

        dw_ref[...] = unpack((frecv[0] + frecv[1]) + (frecv[2] + frecv[3]))

    for i in range(4):
        x2 = (xc + i) % 4
        if i:
            pl.when(core == root)(lambda x2=x2: to_even(x2).wait_send())
        else:
            pl.when((core == root) & (core == 1))(lambda x2=x2: to_even(x2).wait_send())

    @pl.when((root == 0) & (core == 0))
    def _():
        to_odd().wait_send()

    def drain(j, carry):
        @pl.when((4 * core + j - z + 8) % 8 != 0)
        def _():
            for i in range(4):
                pltpu.make_async_remote_copy(
                    src_ref=sbuf.at[j, i], dst_ref=ra.at[j, i], send_sem=ssem.at[j, i],
                    recv_sem=rasem.at[j, i], device_id={"gy": (z + 1) % 8}, device_id_type=MESH).wait_send()

        return carry

    lax.fori_loop(0, 4, drain, 0)
    for j in range(4):
        pl.when(4 * core + j != z)(lambda j=j: straight(j).wait_send())
    for j in range(4):
        long_in(j).wait_send()
        root_in(j, 1).wait_send()
        root_in(j, 3).wait_send()
    pl.when(s > 0)(lambda: ycopy.wait_send())

    @pl.when(s < 3)
    def _():
        ycopy.wait_recv()
        up_ref[...] = lrecv[...]

    @pl.when(s == 3)
    def _():
        up_ref[...] = jnp.zeros((512, 320), BF16)


def finish(up_in, dw_in, par_in, up_ref, dw_ref, par_ref):
    up_ref[...] = up_in[...]
    dw_ref[...] = dw_in[...].reshape(135, 1, 320)
    par_ref[...] = par_in[...].reshape(3, 1, 320)


def local(level_input, out_grad, conv_weight, norm_gain, norm_shift):
    vm = pl.BlockSpec(memory_space=pltpu.VMEM)
    dma = pltpu.SemaphoreType.DMA
    V = pltpu.VMEM
    up, dw, par = pl.pallas_call(
        kernel,
        out_shape=(V((512, 320), BF16), V((135, 320), F32), V((3, 320), F32)),
        in_specs=[vm, vm, pl.BlockSpec(memory_space=pl.ANY), vm, vm],
        out_specs=(vm, vm, vm),
        scratch_shapes=[
            V((27, 320, 320), BF16), V((3, 6, 160, 320), BF16), V((3, 6, 160, 320), BF16),
            V((4, 3, 160, 128), F32), V((2, 160, 128), F32),
            V((2, 4, 3, 16, 128), F32), V((4, 3, 16, 128), F32), V((4, 3, 16, 128), F32),
            V((8, 320), F32), V((8, 8, 320), F32), V((8, 320), F32), V((8, 8, 320), F32),
            V((8, 320), F32), V((8, 8, 320), F32), V((8, 320), F32), V((8, 8, 320), F32),
            V((512, 320), BF16), V((512, 320), BF16), V((320, 1024), BF16),
            V((512, 320), F32), V((512, 320), F32), V((512, 320), F32), V((14 * 320 + 8, 320), F32), V((4, 8, 176, 256), F32),
            V((4, 4, 176, 256), BF16), V((4, 4, 176, 256), BF16), V((4, 4, 176, 256), BF16),
            V((4, 176, 256), F32), V((4, 176, 256), BF16), V((8, 176, 256), BF16),
            V((4, 3, 176, 256), BF16), V((4, 176, 256), BF16), V((4, 2, 176, 256), BF16),
            V((4, 176, 256), F32), V((4, 176, 256), F32), V((176, 256), F32), V((176, 256), F32),
            V((512, 320), BF16), V((512, 320), BF16),
            dma(()), dma((2,)), dma((2,)), dma((2,)), dma((2,)), dma(()), dma(()), dma(()), dma(()),
            dma((8,)), dma((8,)), dma((8,)), dma((8,)), dma((8,)), dma((8,)), dma((8,)), dma((8,)),
            dma((4, 4)), dma((4, 4)), dma((4, 4)), dma((4,)), dma((8,)), dma((4, 3)), dma((4,)), dma((4, 2)),
            dma((4,)), dma((4,)), dma(()), dma(()), dma(()), dma(()),
        ],
        compiler_params=pltpu.CompilerParams(
            collective_id=0, has_side_effects=True, vmem_limit_bytes=60 * 1024 * 1024
        ),
    )(
        level_input.reshape(512, 320), out_grad.reshape(4, 128, 320), conv_weight.reshape(27, 320, 320),
        norm_gain, norm_shift,
    )
    up, dw, par = pl.pallas_call(
        finish,
        out_shape=(
            jax.ShapeDtypeStruct((512, 320), BF16),
            jax.ShapeDtypeStruct((135, 1, 320), F32),
            jax.ShapeDtypeStruct((3, 1, 320), F32),
        ),
        in_specs=[vm, vm, vm],
        out_specs=(vm, vm, vm),
        compiler_params=pltpu.CompilerParams(vmem_limit_bytes=8 * 1024 * 1024),
    )(*(pltpu.with_memory_space_constraint(v, pltpu.VMEM) for v in (up, dw, par)))
    return up.reshape(1, 4, 8, 16, 320), dw.reshape(1, 135, 320), par.reshape(1, 3, 320)


def solution(mesh):
    return jax.shard_map(
        local,
        mesh=mesh,
        in_specs=(
            P("section", None, "gy", "gx", None),
            P("section", None, "gy", "gx", None),
            P("section", None, None, None),
            P("section", None),
            P("section", None),
        ),
        out_specs=(
            P("section", None, "gy", "gx", None),
            P("section", ("gy", "gx"), None),
            P("section", None, None),
        ),
        check_vma=False,
    )
```

```python
import jax
import jax.numpy as jnp
from jax import lax
from jax.experimental import pallas as pl
from jax.experimental.pallas import tpu as pltpu
from jax.sharding import PartitionSpec as P

G = 32
EPS = 1e-05
MESH = pl.DeviceIdType.MESH
SLAB = 1080
F32 = jnp.float32
BF16 = jnp.bfloat16


def pack(u):
    rem = u[:, 256:320]
    wide = jnp.concatenate([rem[0:72], jnp.concatenate([rem[72:136], jnp.zeros((8, 64), F32)], axis=0)], axis=1)
    low = jnp.concatenate([wide[40:72], jnp.zeros((8, 128), F32)], axis=0)
    return u[:, 0:256], jnp.concatenate([wide[0:40], low], axis=1)


def unpack(t):
    q = t[136:176]
    wide = jnp.concatenate([q[:, 0:128], q[0:32, 128:256]], axis=0)
    rem = jnp.concatenate([wide[:, 0:64], wide[0:64, 64:128]], axis=0)
    return jnp.concatenate([t[0:136], rem], axis=1)[0:135]


def kernel(x_ref, g_ref, w_hbm, gain_ref, shift_ref,
           up_ref, dw_ref, par_ref,
           wbuf, gs, pgs, gf, tmp, edge_out, edge_l, edge_r, corner_out, corner_in,
           st_x, rx_sx, st_z, rx_sz, pa_x, rx_px, pa_z, rx_pz,
           unit_own, unit_par, unit_t, acc, normed_b, slope_b, part, own,
           sbuf, ra, rb, bown, bs, bra, xs, xm, xr, fsend, frecv, bfin, brecv, lsend, lrecv,
           wsem, zsem, zrsem, esem, ersem, csem, crsem, gsem, grsem, usem, ursem,
           sxs, sxr, szs, szr, pxs, pxr, pzs, pzr,
           ssem, rasem, rbsem, bssem, brasem, xssem, xmsem, xrsem,
           fsem, frsem, bfsem, bfrsem, ysem, yrsem):
    s = lax.axis_index("section")
    z = lax.axis_index("gy")
    me = lax.axis_index("gx")
    core = me % 2
    xc = me // 2
    partner = xc * 2 + 1 - core

    wcopy = pltpu.make_async_copy(w_hbm, wbuf, wsem)
    wcopy.start()

    barrier = pltpu.get_barrier_semaphore()
    for d in range(1, 8):
        pl.semaphore_signal(barrier, inc=1, device_id={"gx": (me + d) % 8}, device_id_type=MESH)
        pl.semaphore_signal(barrier, inc=1, device_id={"gy": (z + d) % 8}, device_id_type=MESH)

    @pl.when(s > 0)
    def _():
        pl.semaphore_signal(barrier, inc=1, device_id={"section": s - 1}, device_id_type=MESH)

    @pl.when(s < 3)
    def _():
        pl.semaphore_signal(barrier, inc=1, device_id={"section": s + 1}, device_id_type=MESH)

    for side in range(2):
        for vert in range(2):
            nx, nz = me + 2 * side - 1, z + 2 * vert - 1

            @pl.when((nx >= 0) & (nx < 8) & (nz >= 0) & (nz < 8))
            def _(nx=nx, nz=nz):
                pl.semaphore_signal(barrier, inc=1, device_id={"gx": nx, "gy": nz}, device_id_type=MESH)

    def stat_body(i, carry):
        a, b = carry
        v = x_ref[pl.ds(pl.multiple_of(i * 64, 64), 64), :].astype(F32)
        return a + jnp.sum(v.reshape(8, 8, 320), axis=0), b + jnp.sum((v * v).reshape(8, 8, 320), axis=0)

    zero8 = jnp.zeros((8, 320), F32)
    a, b = lax.fori_loop(0, 8, stat_body, (zero8, zero8))
    st_x[...] = zero8
    st_x[0:1, :] = jnp.sum(a, axis=0, keepdims=True)
    st_x[1:2, :] = jnp.sum(b, axis=0, keepdims=True)

    zrow = jnp.zeros((4, 16, 320), BF16)
    part[14 * 320:14 * 320 + 8, :] = zero8
    for c in range(3):
        pgs[c, 0] = jnp.zeros((160, 320), BF16)
        pgs[c, 5] = jnp.zeros((160, 320), BF16)
        gs[c, 0] = jnp.zeros((160, 320), BF16)
        gs[c, 5] = jnp.zeros((160, 320), BF16)

    @pl.when(z == 0)
    def _():
        gs[1, 1:5, 0:16, :] = zrow

    @pl.when(z == 7)
    def _():
        gs[1, 1:5, 144:160, :] = zrow

    @pl.when(me == 0)
    def _():
        edge_l[...] = jnp.zeros((4, 3, 8, 128), F32)

    @pl.when(me == 7)
    def _():
        edge_r[...] = jnp.zeros((4, 3, 8, 128), F32)

    def lanes(v, l):
        if l < 2:
            return v[:, 128 * l:128 * l + 128]
        return jnp.concatenate([v[:, 256:320], jnp.zeros((v.shape[0], 64), F32)], axis=1)

    bsum = jnp.zeros((1, 320), F32)
    corner_out[...] = jnp.zeros((2, 2, 3, 8, 128), F32)
    for f in range(4):
        v = g_ref[f]
        gs[1, 1 + f, 16:144, :] = v
        v = v.astype(F32)
        bsum = bsum + jnp.sum(v, axis=0, keepdims=True)
        for l in range(3):
            gf[f, l] = lanes(v, l)
            for side in range(2):
                edge_out[side, f, l] = gf[f, l, pl.ds(15 * side, 8, stride=16), :]
                corner_out[side, 0, l, f:f + 1, :] = gf[f, l, 15 * side:15 * side + 1, :]
                corner_out[side, 1, l, f:f + 1, :] = gf[f, l, 112 + 15 * side:113 + 15 * side, :]
    pa_x[...] = zero8
    pa_x[2:3, :] = bsum

    def corner(side, vert):
        nx, nz = me + 2 * side - 1, z + 2 * vert - 1
        fx, fz = me - 2 * side + 1, z - 2 * vert + 1
        sent = (nx >= 0) & (nx < 8) & (nz >= 0) & (nz < 8)
        due = (fx >= 0) & (fx < 8) & (fz >= 0) & (fz < 8)
        copy = pltpu.make_async_remote_copy(
            src_ref=corner_out.at[side, vert], dst_ref=corner_in.at[side, vert],
            send_sem=csem.at[side, vert], recv_sem=crsem.at[side, vert],
            device_id={"gx": jnp.clip(nx, 0, 7), "gy": jnp.clip(nz, 0, 7)}, device_id_type=MESH)
        return sent, due, copy

    corners = [corner(side, vert) for side in range(2) for vert in range(2)]
    for q in range(4):
        @pl.when(jnp.logical_not(corners[q][1]))
        def _(q=q):
            corner_in[q // 2, q % 2] = jnp.zeros((3, 8, 128), F32)

    wide = jnp.where(me > 0, 1, 0) + jnp.where(me < 7, 1, 0)
    tall = jnp.where(z > 0, 1, 0) + jnp.where(z < 7, 1, 0)
    pl.semaphore_wait(barrier, 14 + jnp.where(s > 0, 1, 0) + jnp.where(s < 3, 1, 0) + wide * tall)

    def gather(src, dst, ssems, rsems, axis, at):
        out = []
        for d in range(1, 8):
            to = (at + d) % 8
            out.append(pltpu.make_async_remote_copy(
                src_ref=src, dst_ref=dst.at[at], send_sem=ssems.at[d], recv_sem=rsems.at[at],
                device_id={axis: to}, device_id_type=MESH))
            out[-1].start()
        dst[pl.ds(at, 1)] = src[...][None]

    def gathered(src, dst, ssems, rsems, axis, at):
        for d in range(1, 8):
            frm = (at + d) % 8
            cp = pltpu.make_async_remote_copy(
                src_ref=src, dst_ref=dst.at[frm], send_sem=ssems.at[d], recv_sem=rsems.at[frm],
                device_id={axis: frm}, device_id_type=MESH)
            cp.wait_send()
            cp.wait_recv()
        tot = dst[0]
        for d in range(1, 8):
            tot = tot + dst[d]
        return tot

    def halo(src_row, dst_row, to, i):
        return pltpu.make_async_remote_copy(
            src_ref=g_ref.at[:, pl.ds(src_row, 16), :],
            dst_ref=gs.at[1, pl.ds(1, 4), pl.ds(dst_row, 16), :],
            send_sem=zsem.at[i], recv_sem=zrsem.at[i], device_id={"gy": to}, device_id_type=MESH)

    gather(st_x, rx_sx, sxs, sxr, "gx", me)
    up_halo = halo(0, 144, jnp.maximum(z - 1, 0), 0)
    down_halo = halo(112, 0, jnp.minimum(z + 1, 7), 1)
    pl.when(z > 0)(lambda: up_halo.start())
    pl.when(z < 7)(lambda: down_halo.start())
    to_left = pltpu.make_async_remote_copy(
        src_ref=edge_out.at[0], dst_ref=edge_r, send_sem=esem.at[0], recv_sem=ersem.at[0],
        device_id={"gx": jnp.maximum(me - 1, 0)}, device_id_type=MESH)
    to_right = pltpu.make_async_remote_copy(
        src_ref=edge_out.at[1], dst_ref=edge_l, send_sem=esem.at[1], recv_sem=ersem.at[1],
        device_id={"gx": jnp.minimum(me + 1, 7)}, device_id_type=MESH)
    pl.when(me > 0)(lambda: to_left.start())
    pl.when(me < 7)(lambda: to_right.start())
    for sent, _, copy in corners:
        pl.when(sent)(lambda copy=copy: copy.start())

    st_z[...] = gathered(st_x, rx_sx, sxs, sxr, "gx", me)
    gather(st_z, rx_sz, szs, szr, "gy", z)

    @pl.when(z > 0)
    def _():
        up_halo.wait_send()
        down_halo.wait_recv()

    @pl.when(z < 7)
    def _():
        down_halo.wait_send()
        up_halo.wait_recv()

    @pl.when(me > 0)
    def _():
        to_left.wait_send()
        to_right.wait_recv()

    @pl.when(me < 7)
    def _():
        to_right.wait_send()
        to_left.wait_recv()

    for sent, due, copy in corners:
        pl.when(sent)(lambda copy=copy: copy.wait_send())
        pl.when(due)(lambda copy=copy: copy.wait_recv())

    for f in range(4):
        ext = gs[1, 1 + f].astype(F32)
        for l in range(3):
            w = 128 if l < 2 else 64
            v = lanes(ext, l)
            tmp[0] = pltpu.roll(v, 1, 0)
            tmp[1] = pltpu.roll(v, 159, 0)
            tmp[0, pl.ds(16, 8, stride=16), :] = edge_l[f, l]
            tmp[1, pl.ds(31, 8, stride=16), :] = edge_r[f, l]
            tmp[0, 0:1, :] = corner_in[1, 1, l, f:f + 1, :]
            tmp[0, 144:145, :] = corner_in[1, 0, l, f:f + 1, :]
            tmp[1, 15:16, :] = corner_in[0, 1, l, f:f + 1, :]
            tmp[1, 159:160, :] = corner_in[0, 0, l, f:f + 1, :]
            gs[2, 1 + f, :, 128 * l:128 * l + w] = tmp[0, :, 0:w].astype(BF16)
            gs[0, 1 + f, :, 128 * l:128 * l + w] = tmp[1, :, 0:w].astype(BF16)
    swap = pltpu.make_async_remote_copy(
        src_ref=gs.at[:, pl.ds(1, 4)], dst_ref=pgs.at[:, pl.ds(1, 4)], send_sem=gsem, recv_sem=grsem,
        device_id={"gx": partner}, device_id_type=MESH)
    swap.start()

    def window(ref, c, a, b):
        v = ref[c, pl.ds(2 - a, 4), pl.ds(pl.multiple_of((2 - b) * 16, 16), 128), :]
        return v.reshape(512, 320)

    def side(ab, carry):
        a, b = ab // 3, ab % 3
        tot = None
        for c in range(3):
            wk = wbuf[ab * 3 + c]
            d = lax.dot_general(window(gs, c, a, b), wk, (((1,), (1,)), ((), ())), preferred_element_type=F32)
            tot = d if tot is None else tot + d
        acc[...] += tot
        return carry

    def sides(lo, hi):
        lax.fori_loop(lo, hi, side, 0)

    acc[...] = jnp.zeros((512, 320), F32)
    wcopy.wait()
    sides(0, 2)
    ia = jnp.floor((lax.broadcasted_iota(jnp.int32, (320, 320), 0).astype(F32) + 0.5) * 0.1)
    ib = jnp.floor((lax.broadcasted_iota(jnp.int32, (320, 320), 1).astype(F32) + 0.5) * 0.1)
    grp = jnp.where(ia == ib, 1.0, 0.0).astype(F32)
    members = float(512 * 64 * 10)
    tot = gathered(st_z, rx_sz, szs, szr, "gy", z)
    per = jnp.dot(tot, grp, precision=lax.Precision.HIGHEST, preferred_element_type=F32) / members
    mean = per[0:1, :]
    var = per[1:2, :] - mean * mean
    inv = 1.0 / jnp.sqrt(var + EPS)
    gain = gain_ref[...]
    shift = shift_ref[...]

    def act_body(i, carry):
        rows = pl.ds(pl.multiple_of(i * 64, 64), 64)
        n = (x_ref[rows, :].astype(F32) - mean) * inv
        y = n * gain + shift
        sg = jax.nn.sigmoid(y)
        unit_own[rows, :] = (y * sg).astype(BF16)
        slope_b[rows, :] = sg * (1.0 + y * (1.0 - sg))
        normed_b[rows, :] = n
        return carry

    lax.fori_loop(0, 8, act_body, 0)
    swap_u = pltpu.make_async_remote_copy(
        src_ref=unit_own, dst_ref=unit_par, send_sem=usem, recv_sem=ursem,
        device_id={"gx": partner}, device_id_type=MESH)
    swap_u.start()
    unit_t[:, 0:512] = unit_own[...].T
    sides(2, 4)
    swap.wait()
    swap_u.wait()
    unit_t[:, 512:1024] = unit_par[...].T

    def taps(u, carry):
        t = jnp.where((4 * core - z + 9) % 8 < 4, 13 - u, u)
        k = 13 * core + t
        ab = k // 3
        c = k % 3
        b = ab % 3
        rows = pl.ds(pl.multiple_of((2 - b) * 16, 16), 128)
        out = pl.ds(pl.multiple_of(t * 320, 64), 320)
        for a in range(3):
            f0, n = max(0, a - 1), 4 - abs(a - 1)

            @pl.when(ab // 3 == a)
            def _(a=a, f0=f0, n=n):
                wins = [ref[c, pl.ds(f0 + 2 - a, n), rows, :].reshape(n * 128, 320) for ref in (gs, pgs)]
                units = [unit_t[:, 512 * i + 128 * f0:512 * i + 128 * (f0 + n)] for i in range(2)]
                part[out, :] = jnp.dot(
                    jnp.concatenate(units, axis=1), jnp.concatenate(wins, axis=0), preferred_element_type=F32)

        return carry


    def packing(j, carry):
        for d in range(8):
            lo = (135 * d) // 8 * 8
            v = part[pl.ds(pl.multiple_of(160 * core + SLAB * j + lo, 8), 144), :]
            main, rest = pack(v[135 * d - lo:135 * d - lo + 136, :])
            own[j, d, 0:136, :] = main
            own[j, d, 136:176, :] = rest
        return carry

    def relay(j, tau, top, mine, sb, up_in, down_in, s_send, s_up, s_down, result):
        delta = (4 * core + j - z + 8) % 8
        going_up = (delta >= 1) & (delta <= top)
        going_down = delta > top

        def sends_up():
            return pltpu.make_async_remote_copy(
                src_ref=sb, dst_ref=up_in, send_sem=s_send, recv_sem=s_up,
                device_id={"gy": (z + 1) % 8}, device_id_type=MESH)

        def sends_down():
            return pltpu.make_async_remote_copy(
                src_ref=sb, dst_ref=down_in, send_sem=s_send, recv_sem=s_down,
                device_id={"gy": (z + 7) % 8}, device_id_type=MESH)

        for cond, when, send, got in (
            (going_up, top - delta, sends_up, up_in),
            (going_down, delta - top - 1, sends_down, down_in),
        ):
            @pl.when(cond & (when == tau))
            def _(send=send, got=got):
                if tau == 0:
                    sb[...] = mine[...].astype(sb.dtype)
                else:
                    send().wait_recv()
                    sb[...] = (mine[...] + got[...].astype(F32)).astype(sb.dtype)
                send().start()

        if tau == 4:
            @pl.when(delta == 0)
            def _():
                sends_up().wait_recv()
                sends_down().wait_recv()
                result[...] = mine[...] + up_in[...].astype(F32) + down_in[...].astype(F32)

    def slab_a(j, tau):
        for i in range(4):
            relay(j, tau, 4 - i % 2, own.at[j, 2 * i], sbuf.at[j, i], ra.at[j, i], rb.at[j, i],
                  ssem.at[j, i], rasem.at[j, i], rbsem.at[j, i], fsend.at[i])

    def chain_a(tau):
        def one(j, carry):
            slab_a(j, tau)
            return carry

        lax.fori_loop(0, 4, one, 0)

    def straight(j):
        return pltpu.make_async_remote_copy(
            src_ref=bs.at[j], dst_ref=bra.at[z], send_sem=bssem.at[j], recv_sem=brasem.at[z],
            device_id={"gy": 4 * core + j}, device_id_type=MESH)

    def straight_sends():
        for j in range(4):
            @pl.when(4 * core + j != z)
            def _(j=j):
                bs[j] = bown[j].astype(BF16)
                straight(j).start()

    def straight_sum():
        @pl.when(core == z // 4)
        def _():
            tot = bown[z - 4 * core]
            for d in range(1, 8):
                frm = (z + d) % 8
                pltpu.make_async_remote_copy(
                    src_ref=bs.at[0], dst_ref=bra.at[frm], send_sem=bssem.at[0], recv_sem=brasem.at[frm],
                    device_id={"gy": frm}, device_id_type=MESH).wait_recv()
                tot = tot + bra[frm].astype(F32)
            bfin[...] = tot

    def ring(j, e, dst, rsem):
        plus = e == 1 or (e == 2 and j % 2 == 0)
        to = ((xc + (1 if plus else 3)) % 4) * 2 + core
        return pltpu.make_async_remote_copy(
            src_ref=xs.at[j, e - 1], dst_ref=dst, send_sem=xssem.at[j, e - 1], recv_sem=rsem,
            device_id={"gx": to}, device_id_type=MESH)

    def odd(j, e):
        return own[j, 2 * ((xc + e) % 4) + 1]

    def long_in(j):
        return ring(j, 2, xm.at[j], xmsem.at[j])

    def root_in(j, e):
        return ring(j, e, xr.at[j, e // 2], xrsem.at[j, e // 2])

    def ring_0(j):
        xs[j, 1] = odd(j, 2).astype(BF16)
        long_in(j).start()
        e = 3 if j % 2 == 0 else 1
        xs[j, e - 1] = odd(j, e).astype(BF16)
        root_in(j, e).start()

    def ring_1():
        for j in range(4):
            e = 1 if j % 2 == 0 else 3
            long_in(j).wait_recv()
            xs[j, e - 1] = (odd(j, e) + xm[j].astype(F32)).astype(BF16)
            root_in(j, e).start()

    def ring_2():
        for j in range(4):
            root_in(j, 1).wait_recv()
            root_in(j, 3).wait_recv()
            bown[j] = odd(j, 0) + xr[j, 0].astype(F32) + xr[j, 1].astype(F32)

    late = (4 * core - z + 9) % 8 < 4
    for i, (t0, t1) in enumerate(((0, 4), (4, 8), (8, 11), (11, 14))):
        lax.fori_loop(t0, t1, taps, 0)
        jd = jnp.where(late, 3 - i, i)
        packing(jd, 0)
        slab_a(jd, 0)
        pl.when(late)(lambda i=i: ring_0(3 - i))
        pl.when(jnp.logical_not(late))(lambda i=i: ring_0(i))

    def grad_body(i, carry):
        p0, p1 = carry
        rows = pl.ds(pl.multiple_of(i * 64, 64), 64)
        ag = acc[rows, :] * slope_b[rows, :]
        acc[rows, :] = ag
        return (p0 + jnp.sum((ag * normed_b[rows, :]).reshape(8, 8, 320), axis=0),
                p1 + jnp.sum(ag.reshape(8, 8, 320), axis=0))

    chain_a(1)
    sides(4, 7)
    ring_1()
    sides(7, 9)
    p0, p1 = lax.fori_loop(0, 8, grad_body, (zero8, zero8))
    pa_x[0:1, :] = jnp.sum(p0, axis=0, keepdims=True)
    pa_x[1:2, :] = jnp.sum(p1, axis=0, keepdims=True)
    gather(pa_x, rx_px, pxs, pxr, "gx", me)
    chain_a(2)
    pa_z[...] = gathered(pa_x, rx_px, pxs, pxr, "gx", me)
    gather(pa_z, rx_pz, pzs, pzr, "gy", z)
    chain_a(3)
    ring_2()
    straight_sends()

    ptot = gathered(pa_z, rx_pz, pzs, pzr, "gy", z)
    par_ref[...] = ptot[0:3, :]
    gg = jnp.dot(ptot * gain, grp, precision=lax.Precision.HIGHEST, preferred_element_type=F32) / members
    second = gg[0:1, :]
    first = gg[1:2, :]

    def lev(i, carry):
        rows = pl.ds(pl.multiple_of(i * 64, 64), 64)
        gv = g_ref[i // 2, pl.ds(pl.multiple_of((i % 2) * 64, 64), 64), :].astype(F32)
        ng = (acc[rows, :] * gain - first - normed_b[rows, :] * second) * inv
        lsend[rows, :] = (gv + ng).astype(BF16)
        return carry

    lax.fori_loop(0, 8, lev, 0)
    ycopy = pltpu.make_async_remote_copy(
        src_ref=lsend, dst_ref=lrecv, send_sem=ysem, recv_sem=yrsem,
        device_id={"section": jnp.maximum(s - 1, 0)}, device_id_type=MESH)
    pl.when(s > 0)(lambda: ycopy.start())

    chain_a(4)

    root = z // 4

    def to_even(x2):
        return pltpu.make_async_remote_copy(
            src_ref=fsend.at[x2], dst_ref=frecv.at[xc], send_sem=fsem.at[x2], recv_sem=frsem.at[xc],
            device_id={"gx": 2 * x2}, device_id_type=MESH)

    def to_odd():
        return pltpu.make_async_remote_copy(
            src_ref=bfin, dst_ref=brecv, send_sem=bfsem, recv_sem=bfrsem,
            device_id={"gx": partner}, device_id_type=MESH)

    for i in range(4):
        x2 = (xc + i) % 4
        if i:
            pl.when(core == root)(lambda x2=x2: to_even(x2).start())
        else:
            pl.when((core == root) & (core == 1))(lambda x2=x2: to_even(x2).start())

            @pl.when((core == root) & (core == 0))
            def _():
                frecv[pl.ds(xc, 1)] = fsend[pl.ds(xc, 1)]

    straight_sum()

    @pl.when((root == 0) & (core == 0))
    def _():
        to_odd().start()

    @pl.when((root == 1) & (core == 1))
    def _():
        dw_ref[...] = unpack(bfin[...])

    @pl.when((root == 0) & (core == 1))
    def _():
        to_odd().wait_recv()
        dw_ref[...] = unpack(brecv[...])

    @pl.when(core == 0)
    def _():
        for q in range(4):
            @pl.when((root == 1) | (xc != q))
            def _(q=q):
                pltpu.make_async_remote_copy(
                    src_ref=fsend.at[q], dst_ref=frecv.at[q], send_sem=fsem.at[q], recv_sem=frsem.at[q],
                    device_id={"gx": partner}, device_id_type=MESH).wait_recv()

        dw_ref[...] = unpack((frecv[0] + frecv[1]) + (frecv[2] + frecv[3]))

    for i in range(4):
        x2 = (xc + i) % 4
        if i:
            pl.when(core == root)(lambda x2=x2: to_even(x2).wait_send())
        else:
            pl.when((core == root) & (core == 1))(lambda x2=x2: to_even(x2).wait_send())

    @pl.when((root == 0) & (core == 0))
    def _():
        to_odd().wait_send()

    def drain(j, carry):
        @pl.when((4 * core + j - z + 8) % 8 != 0)
        def _():
            for i in range(4):
                pltpu.make_async_remote_copy(
                    src_ref=sbuf.at[j, i], dst_ref=ra.at[j, i], send_sem=ssem.at[j, i],
                    recv_sem=rasem.at[j, i], device_id={"gy": (z + 1) % 8}, device_id_type=MESH).wait_send()

        return carry

    lax.fori_loop(0, 4, drain, 0)
    for j in range(4):
        pl.when(4 * core + j != z)(lambda j=j: straight(j).wait_send())
    for j in range(4):
        long_in(j).wait_send()
        root_in(j, 1).wait_send()
        root_in(j, 3).wait_send()
    pl.when(s > 0)(lambda: ycopy.wait_send())

    @pl.when(s < 3)
    def _():
        ycopy.wait_recv()
        up_ref[...] = lrecv[...]

    @pl.when(s == 3)
    def _():
        up_ref[...] = jnp.zeros((512, 320), BF16)


def finish(up_in, dw_in, par_in, up_ref, dw_ref, par_ref):
    up_ref[...] = up_in[...]
    dw_ref[...] = dw_in[...].reshape(135, 1, 320)
    par_ref[...] = par_in[...].reshape(3, 1, 320)


def local(level_input, out_grad, conv_weight, norm_gain, norm_shift):
    vm = pl.BlockSpec(memory_space=pltpu.VMEM)
    dma = pltpu.SemaphoreType.DMA
    V = pltpu.VMEM
    up, dw, par = pl.pallas_call(
        kernel,
        out_shape=(V((512, 320), BF16), V((135, 320), F32), V((3, 320), F32)),
        in_specs=[vm, vm, pl.BlockSpec(memory_space=pl.ANY), vm, vm],
        out_specs=(vm, vm, vm),
        scratch_shapes=[
            V((27, 320, 320), BF16), V((3, 6, 160, 320), BF16), V((3, 6, 160, 320), BF16),
            V((4, 3, 128, 128), F32), V((2, 160, 128), F32),
            V((2, 4, 3, 8, 128), F32), V((4, 3, 8, 128), F32), V((4, 3, 8, 128), F32),
            V((2, 2, 3, 8, 128), F32), V((2, 2, 3, 8, 128), F32),
            V((8, 320), F32), V((8, 8, 320), F32), V((8, 320), F32), V((8, 8, 320), F32),
            V((8, 320), F32), V((8, 8, 320), F32), V((8, 320), F32), V((8, 8, 320), F32),
            V((512, 320), BF16), V((512, 320), BF16), V((320, 1024), BF16),
            V((512, 320), F32), V((512, 320), F32), V((512, 320), F32), V((14 * 320 + 8, 320), F32), V((4, 8, 176, 256), F32),
            V((4, 4, 176, 256), BF16), V((4, 4, 176, 256), BF16), V((4, 4, 176, 256), BF16),
            V((4, 176, 256), F32), V((4, 176, 256), BF16), V((8, 176, 256), BF16),
            V((4, 3, 176, 256), BF16), V((4, 176, 256), BF16), V((4, 2, 176, 256), BF16),
            V((4, 176, 256), F32), V((4, 176, 256), F32), V((176, 256), F32), V((176, 256), F32),
            V((512, 320), BF16), V((512, 320), BF16),
            dma(()), dma((2,)), dma((2,)), dma((2,)), dma((2,)), dma((2, 2)), dma((2, 2)), dma(()), dma(()), dma(()), dma(()),
            dma((8,)), dma((8,)), dma((8,)), dma((8,)), dma((8,)), dma((8,)), dma((8,)), dma((8,)),
            dma((4, 4)), dma((4, 4)), dma((4, 4)), dma((4,)), dma((8,)), dma((4, 3)), dma((4,)), dma((4, 2)),
            dma((4,)), dma((4,)), dma(()), dma(()), dma(()), dma(()),
        ],
        compiler_params=pltpu.CompilerParams(
            collective_id=0, has_side_effects=True, vmem_limit_bytes=60 * 1024 * 1024
        ),
    )(
        level_input.reshape(512, 320), out_grad.reshape(4, 128, 320), conv_weight.reshape(27, 320, 320),
        norm_gain, norm_shift,
    )
    up, dw, par = pl.pallas_call(
        finish,
        out_shape=(
            jax.ShapeDtypeStruct((512, 320), BF16),
            jax.ShapeDtypeStruct((135, 1, 320), F32),
            jax.ShapeDtypeStruct((3, 1, 320), F32),
        ),
        in_specs=[vm, vm, vm],
        out_specs=(vm, vm, vm),
        compiler_params=pltpu.CompilerParams(vmem_limit_bytes=8 * 1024 * 1024),
    )(*(pltpu.with_memory_space_constraint(v, pltpu.VMEM) for v in (up, dw, par)))
    return up.reshape(1, 4, 8, 16, 320), dw.reshape(1, 135, 320), par.reshape(1, 3, 320)


def solution(mesh):
    return jax.shard_map(
        local,
        mesh=mesh,
        in_specs=(
            P("section", None, "gy", "gx", None),
            P("section", None, "gy", "gx", None),
            P("section", None, None, None),
            P("section", None),
            P("section", None),
        ),
        out_specs=(
            P("section", None, "gy", "gx", None),
            P("section", ("gy", "gx"), None),
            P("section", None, None),
        ),
        check_vma=False,
    )
```

```python
import jax
import jax.numpy as jnp
from jax import lax
from jax.experimental import pallas as pl
from jax.experimental.pallas import tpu as pltpu
from jax.sharding import PartitionSpec as P

G = 32
EPS = 1e-05
MESH = pl.DeviceIdType.MESH
SLAB = 1080
F32 = jnp.float32
BF16 = jnp.bfloat16


def pack(u):
    rem = u[:, 256:320]
    wide = jnp.concatenate([rem[0:72], jnp.concatenate([rem[72:136], jnp.zeros((8, 64), F32)], axis=0)], axis=1)
    low = jnp.concatenate([wide[40:72], jnp.zeros((8, 128), F32)], axis=0)
    return u[:, 0:256], jnp.concatenate([wide[0:40], low], axis=1)


def unpack(t):
    q = t[136:176]
    wide = jnp.concatenate([q[:, 0:128], q[0:32, 128:256]], axis=0)
    rem = jnp.concatenate([wide[:, 0:64], wide[0:64, 64:128]], axis=0)
    return jnp.concatenate([t[0:136], rem], axis=1)[0:135]


def kernel(x_ref, g_ref, w_hbm, gain_ref, shift_ref,
           up_ref, dw_ref, par_ref,
           wbuf, gs, pgs, gf, tmp, edge_out, edge_l, edge_r, corner_out, corner_in,
           st_x, rx_sx, st_z, rx_sz, pa_x, rx_px, pa_z, rx_pz,
           unit_own, unit_par, unit_t, acc, normed_b, slope_b, part, own,
           sbuf, ra, rb, bown, bs, bra, xs, xm, xr, fsend, frecv, bfin, brecv, lsend, lrecv,
           wsem, zsem, zrsem, esem, ersem, csem, crsem, gsem, grsem, usem, ursem,
           sxs, sxr, szs, szr, pxs, pxr, pzs, pzr,
           ssem, rasem, rbsem, bssem, brasem, xssem, xmsem, xrsem,
           fsem, frsem, bfsem, bfrsem, ysem, yrsem):
    s = lax.axis_index("section")
    z = lax.axis_index("gy")
    me = lax.axis_index("gx")
    core = me % 2
    xc = me // 2
    partner = xc * 2 + 1 - core

    wcopy = pltpu.make_async_copy(w_hbm, wbuf, wsem)
    wcopy.start()

    barrier = pltpu.get_barrier_semaphore()
    for d in range(1, 8):
        pl.semaphore_signal(barrier, inc=1, device_id={"gx": (me + d) % 8}, device_id_type=MESH)
        pl.semaphore_signal(barrier, inc=1, device_id={"gy": (z + d) % 8}, device_id_type=MESH)

    @pl.when(s > 0)
    def _():
        pl.semaphore_signal(barrier, inc=1, device_id={"section": s - 1}, device_id_type=MESH)

    @pl.when(s < 3)
    def _():
        pl.semaphore_signal(barrier, inc=1, device_id={"section": s + 1}, device_id_type=MESH)

    for side in range(2):
        for vert in range(2):
            nx, nz = me + 2 * side - 1, z + 2 * vert - 1

            @pl.when((nx >= 0) & (nx < 8) & (nz >= 0) & (nz < 8))
            def _(nx=nx, nz=nz):
                pl.semaphore_signal(barrier, inc=1, device_id={"gx": nx, "gy": nz}, device_id_type=MESH)

    def stat_body(i, carry):
        a, b = carry
        v = x_ref[pl.ds(pl.multiple_of(i * 64, 64), 64), :].astype(F32)
        return a + jnp.sum(v.reshape(8, 8, 320), axis=0), b + jnp.sum((v * v).reshape(8, 8, 320), axis=0)

    zero8 = jnp.zeros((8, 320), F32)
    a, b = lax.fori_loop(0, 8, stat_body, (zero8, zero8))
    st_x[...] = zero8
    st_x[0:1, :] = jnp.sum(a, axis=0, keepdims=True)
    st_x[1:2, :] = jnp.sum(b, axis=0, keepdims=True)

    zrow = jnp.zeros((4, 16, 320), BF16)
    part[14 * 320:14 * 320 + 8, :] = zero8
    for c in range(3):
        pgs[c, 0] = jnp.zeros((160, 320), BF16)
        pgs[c, 5] = jnp.zeros((160, 320), BF16)
        gs[c, 0] = jnp.zeros((160, 320), BF16)
        gs[c, 5] = jnp.zeros((160, 320), BF16)

    @pl.when(z == 0)
    def _():
        gs[1, 1:5, 0:16, :] = zrow

    @pl.when(z == 7)
    def _():
        gs[1, 1:5, 144:160, :] = zrow

    @pl.when(me == 0)
    def _():
        edge_l[...] = jnp.zeros((4, 3, 8, 128), F32)

    @pl.when(me == 7)
    def _():
        edge_r[...] = jnp.zeros((4, 3, 8, 128), F32)

    def lanes(v, l):
        if l < 2:
            return v[:, 128 * l:128 * l + 128]
        return jnp.concatenate([v[:, 256:320], jnp.zeros((v.shape[0], 64), F32)], axis=1)

    bsum = jnp.zeros((1, 320), F32)
    corner_out[...] = jnp.zeros((2, 2, 3, 8, 128), F32)
    for f in range(4):
        v = g_ref[f]
        gs[1, 1 + f, 16:144, :] = v
        v = v.astype(F32)
        bsum = bsum + jnp.sum(v, axis=0, keepdims=True)
        for l in range(3):
            gf[f, l] = lanes(v, l)
            for side in range(2):
                edge_out[side, f, l] = gf[f, l, pl.ds(15 * side, 8, stride=16), :]
                corner_out[side, 0, l, f:f + 1, :] = gf[f, l, 15 * side:15 * side + 1, :]
                corner_out[side, 1, l, f:f + 1, :] = gf[f, l, 112 + 15 * side:113 + 15 * side, :]
    pa_x[...] = zero8
    pa_x[2:3, :] = bsum

    def corner(side, vert):
        nx, nz = me + 2 * side - 1, z + 2 * vert - 1
        fx, fz = me - 2 * side + 1, z - 2 * vert + 1
        sent = (nx >= 0) & (nx < 8) & (nz >= 0) & (nz < 8)
        due = (fx >= 0) & (fx < 8) & (fz >= 0) & (fz < 8)
        copy = pltpu.make_async_remote_copy(
            src_ref=corner_out.at[side, vert], dst_ref=corner_in.at[side, vert],
            send_sem=csem.at[side, vert], recv_sem=crsem.at[side, vert],
            device_id={"gx": jnp.clip(nx, 0, 7), "gy": jnp.clip(nz, 0, 7)}, device_id_type=MESH)
        return sent, due, copy

    corners = [corner(side, vert) for side in range(2) for vert in range(2)]
    for q in range(4):
        @pl.when(jnp.logical_not(corners[q][1]))
        def _(q=q):
            corner_in[q // 2, q % 2] = jnp.zeros((3, 8, 128), F32)

    wide = jnp.where(me > 0, 1, 0) + jnp.where(me < 7, 1, 0)
    tall = jnp.where(z > 0, 1, 0) + jnp.where(z < 7, 1, 0)
    pl.semaphore_wait(barrier, 14 + jnp.where(s > 0, 1, 0) + jnp.where(s < 3, 1, 0) + wide * tall)

    def gather(src, dst, ssems, rsems, axis, at):
        out = []
        for d in range(1, 8):
            to = (at + d) % 8
            out.append(pltpu.make_async_remote_copy(
                src_ref=src, dst_ref=dst.at[at], send_sem=ssems.at[d], recv_sem=rsems.at[at],
                device_id={axis: to}, device_id_type=MESH))
            out[-1].start()
        dst[pl.ds(at, 1)] = src[...][None]

    def gathered(src, dst, ssems, rsems, axis, at):
        for d in range(1, 8):
            frm = (at + d) % 8
            cp = pltpu.make_async_remote_copy(
                src_ref=src, dst_ref=dst.at[frm], send_sem=ssems.at[d], recv_sem=rsems.at[frm],
                device_id={axis: frm}, device_id_type=MESH)
            cp.wait_send()
            cp.wait_recv()
        tot = dst[0]
        for d in range(1, 8):
            tot = tot + dst[d]
        return tot

    def halo(src_row, dst_row, to, i):
        return pltpu.make_async_remote_copy(
            src_ref=g_ref.at[:, pl.ds(src_row, 16), :],
            dst_ref=gs.at[1, pl.ds(1, 4), pl.ds(dst_row, 16), :],
            send_sem=zsem.at[i], recv_sem=zrsem.at[i], device_id={"gy": to}, device_id_type=MESH)

    gather(st_x, rx_sx, sxs, sxr, "gx", me)
    up_halo = halo(0, 144, jnp.maximum(z - 1, 0), 0)
    down_halo = halo(112, 0, jnp.minimum(z + 1, 7), 1)
    pl.when(z > 0)(lambda: up_halo.start())
    pl.when(z < 7)(lambda: down_halo.start())
    to_left = pltpu.make_async_remote_copy(
        src_ref=edge_out.at[0], dst_ref=edge_r, send_sem=esem.at[0], recv_sem=ersem.at[0],
        device_id={"gx": jnp.maximum(me - 1, 0)}, device_id_type=MESH)
    to_right = pltpu.make_async_remote_copy(
        src_ref=edge_out.at[1], dst_ref=edge_l, send_sem=esem.at[1], recv_sem=ersem.at[1],
        device_id={"gx": jnp.minimum(me + 1, 7)}, device_id_type=MESH)
    pl.when(me > 0)(lambda: to_left.start())
    pl.when(me < 7)(lambda: to_right.start())
    for sent, _, copy in corners:
        pl.when(sent)(lambda copy=copy: copy.start())

    st_z[...] = gathered(st_x, rx_sx, sxs, sxr, "gx", me)
    gather(st_z, rx_sz, szs, szr, "gy", z)

    @pl.when(z > 0)
    def _():
        up_halo.wait_send()
        down_halo.wait_recv()

    @pl.when(z < 7)
    def _():
        down_halo.wait_send()
        up_halo.wait_recv()

    @pl.when(me > 0)
    def _():
        to_left.wait_send()
        to_right.wait_recv()

    @pl.when(me < 7)
    def _():
        to_right.wait_send()
        to_left.wait_recv()

    for sent, due, copy in corners:
        pl.when(sent)(lambda copy=copy: copy.wait_send())
        pl.when(due)(lambda copy=copy: copy.wait_recv())

    for f in range(4):
        ext = gs[1, 1 + f].astype(F32)
        for l in range(3):
            w = 128 if l < 2 else 64
            v = lanes(ext, l)
            tmp[0] = pltpu.roll(v, 1, 0)
            tmp[1] = pltpu.roll(v, 159, 0)
            tmp[0, pl.ds(16, 8, stride=16), :] = edge_l[f, l]
            tmp[1, pl.ds(31, 8, stride=16), :] = edge_r[f, l]
            tmp[0, 0:1, :] = corner_in[1, 1, l, f:f + 1, :]
            tmp[0, 144:145, :] = corner_in[1, 0, l, f:f + 1, :]
            tmp[1, 15:16, :] = corner_in[0, 1, l, f:f + 1, :]
            tmp[1, 159:160, :] = corner_in[0, 0, l, f:f + 1, :]
            gs[2, 1 + f, :, 128 * l:128 * l + w] = tmp[0, :, 0:w].astype(BF16)
            gs[0, 1 + f, :, 128 * l:128 * l + w] = tmp[1, :, 0:w].astype(BF16)
    swap = pltpu.make_async_remote_copy(
        src_ref=gs.at[:, pl.ds(1, 4)], dst_ref=pgs.at[:, pl.ds(1, 4)], send_sem=gsem, recv_sem=grsem,
        device_id={"gx": partner}, device_id_type=MESH)
    swap.start()

    def window(ref, c, a, b):
        v = ref[c, pl.ds(2 - a, 4), pl.ds(pl.multiple_of((2 - b) * 16, 16), 128), :]
        return v.reshape(512, 320)

    def side(ab, carry):
        b = ab % 3
        rows = pl.ds(pl.multiple_of((2 - b) * 16, 16), 128)
        for a in range(3):
            f0, n = max(0, a - 1), 4 - abs(a - 1)

            @pl.when(ab // 3 == a)
            def _(a=a, f0=f0, n=n):
                tot = None
                for c in range(3):
                    win = gs[c, f0 + 2 - a:f0 + 2 - a + n, rows, :].reshape(n * 128, 320)
                    d = lax.dot_general(
                        win, wbuf[ab * 3 + c], (((1,), (1,)), ((), ())), preferred_element_type=F32)
                    tot = d if tot is None else tot + d
                acc[128 * f0:128 * (f0 + n), :] += tot

        return carry

    def sides(lo, hi):
        lax.fori_loop(lo, hi, side, 0)

    acc[...] = jnp.zeros((512, 320), F32)
    wcopy.wait()
    sides(0, 3)
    ia = jnp.floor((lax.broadcasted_iota(jnp.int32, (320, 320), 0).astype(F32) + 0.5) * 0.1)
    ib = jnp.floor((lax.broadcasted_iota(jnp.int32, (320, 320), 1).astype(F32) + 0.5) * 0.1)
    grp = jnp.where(ia == ib, 1.0, 0.0).astype(F32)
    members = float(512 * 64 * 10)
    tot = gathered(st_z, rx_sz, szs, szr, "gy", z)
    per = jnp.dot(tot, grp, precision=lax.Precision.HIGHEST, preferred_element_type=F32) / members
    mean = per[0:1, :]
    var = per[1:2, :] - mean * mean
    inv = 1.0 / jnp.sqrt(var + EPS)
    gain = gain_ref[...]
    shift = shift_ref[...]

    def act_body(i, carry):
        rows = pl.ds(pl.multiple_of(i * 64, 64), 64)
        n = (x_ref[rows, :].astype(F32) - mean) * inv
        y = n * gain + shift
        sg = jax.nn.sigmoid(y)
        unit_own[rows, :] = (y * sg).astype(BF16)
        slope_b[rows, :] = sg * (1.0 + y * (1.0 - sg))
        normed_b[rows, :] = n
        return carry

    lax.fori_loop(0, 8, act_body, 0)
    swap_u = pltpu.make_async_remote_copy(
        src_ref=unit_own, dst_ref=unit_par, send_sem=usem, recv_sem=ursem,
        device_id={"gx": partner}, device_id_type=MESH)
    swap_u.start()
    unit_t[:, 0:512] = unit_own[...].T
    sides(3, 6)
    swap.wait()
    swap_u.wait()
    unit_t[:, 512:1024] = unit_par[...].T

    def taps(u, carry):
        t = jnp.where((4 * core - z + 9) % 8 < 4, 13 - u, u)
        k = 13 * core + t
        ab = k // 3
        c = k % 3
        b = ab % 3
        rows = pl.ds(pl.multiple_of((2 - b) * 16, 16), 128)
        out = pl.ds(pl.multiple_of(t * 320, 64), 320)
        for a in range(3):
            f0, n = max(0, a - 1), 4 - abs(a - 1)

            @pl.when(ab // 3 == a)
            def _(a=a, f0=f0, n=n):
                wins = [ref[c, pl.ds(f0 + 2 - a, n), rows, :].reshape(n * 128, 320) for ref in (gs, pgs)]
                units = [unit_t[:, 512 * i + 128 * f0:512 * i + 128 * (f0 + n)] for i in range(2)]
                part[out, :] = jnp.dot(
                    jnp.concatenate(units, axis=1), jnp.concatenate(wins, axis=0), preferred_element_type=F32)

        return carry


    def packing(j, carry):
        for d in range(8):
            lo = (135 * d) // 8 * 8
            v = part[pl.ds(pl.multiple_of(160 * core + SLAB * j + lo, 8), 144), :]
            main, rest = pack(v[135 * d - lo:135 * d - lo + 136, :])
            own[j, d, 0:136, :] = main
            own[j, d, 136:176, :] = rest
        return carry

    def relay(j, tau, top, mine, sb, up_in, down_in, s_send, s_up, s_down, result):
        delta = (4 * core + j - z + 8) % 8
        going_up = (delta >= 1) & (delta <= top)
        going_down = delta > top

        def sends_up():
            return pltpu.make_async_remote_copy(
                src_ref=sb, dst_ref=up_in, send_sem=s_send, recv_sem=s_up,
                device_id={"gy": (z + 1) % 8}, device_id_type=MESH)

        def sends_down():
            return pltpu.make_async_remote_copy(
                src_ref=sb, dst_ref=down_in, send_sem=s_send, recv_sem=s_down,
                device_id={"gy": (z + 7) % 8}, device_id_type=MESH)

        for cond, when, send, got in (
            (going_up, top - delta, sends_up, up_in),
            (going_down, delta - top - 1, sends_down, down_in),
        ):
            @pl.when(cond & (when == tau))
            def _(send=send, got=got):
                if tau == 0:
                    sb[...] = mine[...].astype(sb.dtype)
                else:
                    send().wait_recv()
                    sb[...] = (mine[...] + got[...].astype(F32)).astype(sb.dtype)
                send().start()

        if tau == 4:
            @pl.when(delta == 0)
            def _():
                sends_up().wait_recv()
                sends_down().wait_recv()
                result[...] = mine[...] + up_in[...].astype(F32) + down_in[...].astype(F32)

    def slab_a(j, tau):
        for i in range(4):
            relay(j, tau, 4 - i % 2, own.at[j, 2 * i], sbuf.at[j, i], ra.at[j, i], rb.at[j, i],
                  ssem.at[j, i], rasem.at[j, i], rbsem.at[j, i], fsend.at[i])

    def chain_a(tau):
        def one(j, carry):
            slab_a(j, tau)
            return carry

        lax.fori_loop(0, 4, one, 0)

    def straight(j):
        return pltpu.make_async_remote_copy(
            src_ref=bs.at[j], dst_ref=bra.at[z], send_sem=bssem.at[j], recv_sem=brasem.at[z],
            device_id={"gy": 4 * core + j}, device_id_type=MESH)

    def straight_sends():
        for j in range(4):
            @pl.when(4 * core + j != z)
            def _(j=j):
                bs[j] = bown[j].astype(BF16)
                straight(j).start()

    def straight_sum():
        @pl.when(core == z // 4)
        def _():
            tot = bown[z - 4 * core]
            for d in range(1, 8):
                frm = (z + d) % 8
                pltpu.make_async_remote_copy(
                    src_ref=bs.at[0], dst_ref=bra.at[frm], send_sem=bssem.at[0], recv_sem=brasem.at[frm],
                    device_id={"gy": frm}, device_id_type=MESH).wait_recv()
                tot = tot + bra[frm].astype(F32)
            bfin[...] = tot

    def ring(j, e, dst, rsem):
        plus = e == 1 or (e == 2 and j % 2 == 0)
        to = ((xc + (1 if plus else 3)) % 4) * 2 + core
        return pltpu.make_async_remote_copy(
            src_ref=xs.at[j, e - 1], dst_ref=dst, send_sem=xssem.at[j, e - 1], recv_sem=rsem,
            device_id={"gx": to}, device_id_type=MESH)

    def odd(j, e):
        return own[j, 2 * ((xc + e) % 4) + 1]

    def long_in(j):
        return ring(j, 2, xm.at[j], xmsem.at[j])

    def root_in(j, e):
        return ring(j, e, xr.at[j, e // 2], xrsem.at[j, e // 2])

    def ring_0(j):
        xs[j, 1] = odd(j, 2).astype(BF16)
        long_in(j).start()
        e = 3 if j % 2 == 0 else 1
        xs[j, e - 1] = odd(j, e).astype(BF16)
        root_in(j, e).start()

    def ring_1():
        for j in range(4):
            e = 1 if j % 2 == 0 else 3
            long_in(j).wait_recv()
            xs[j, e - 1] = (odd(j, e) + xm[j].astype(F32)).astype(BF16)
            root_in(j, e).start()

    def ring_2():
        for j in range(4):
            root_in(j, 1).wait_recv()
            root_in(j, 3).wait_recv()
            bown[j] = odd(j, 0) + xr[j, 0].astype(F32) + xr[j, 1].astype(F32)

    late = (4 * core - z + 9) % 8 < 4
    for i, (t0, t1) in enumerate(((0, 4), (4, 8), (8, 11), (11, 14))):
        lax.fori_loop(t0, t1, taps, 0)
        jd = jnp.where(late, 3 - i, i)
        packing(jd, 0)
        slab_a(jd, 0)
        pl.when(late)(lambda i=i: ring_0(3 - i))
        pl.when(jnp.logical_not(late))(lambda i=i: ring_0(i))

    def grad_body(i, carry):
        p0, p1 = carry
        rows = pl.ds(pl.multiple_of(i * 64, 64), 64)
        ag = acc[rows, :] * slope_b[rows, :]
        acc[rows, :] = ag
        return (p0 + jnp.sum((ag * normed_b[rows, :]).reshape(8, 8, 320), axis=0),
                p1 + jnp.sum(ag.reshape(8, 8, 320), axis=0))

    chain_a(1)
    sides(6, 8)
    ring_1()
    sides(8, 9)
    p0, p1 = lax.fori_loop(0, 8, grad_body, (zero8, zero8))
    pa_x[0:1, :] = jnp.sum(p0, axis=0, keepdims=True)
    pa_x[1:2, :] = jnp.sum(p1, axis=0, keepdims=True)
    gather(pa_x, rx_px, pxs, pxr, "gx", me)
    chain_a(2)
    pa_z[...] = gathered(pa_x, rx_px, pxs, pxr, "gx", me)
    gather(pa_z, rx_pz, pzs, pzr, "gy", z)
    chain_a(3)
    ring_2()
    straight_sends()

    ptot = gathered(pa_z, rx_pz, pzs, pzr, "gy", z)
    par_ref[...] = ptot[0:3, :]
    gg = jnp.dot(ptot * gain, grp, precision=lax.Precision.HIGHEST, preferred_element_type=F32) / members
    second = gg[0:1, :]
    first = gg[1:2, :]

    def lev(i, carry):
        rows = pl.ds(pl.multiple_of(i * 64, 64), 64)
        gv = g_ref[i // 2, pl.ds(pl.multiple_of((i % 2) * 64, 64), 64), :].astype(F32)
        ng = (acc[rows, :] * gain - first - normed_b[rows, :] * second) * inv
        lsend[rows, :] = (gv + ng).astype(BF16)
        return carry

    lax.fori_loop(0, 8, lev, 0)
    ycopy = pltpu.make_async_remote_copy(
        src_ref=lsend, dst_ref=lrecv, send_sem=ysem, recv_sem=yrsem,
        device_id={"section": jnp.maximum(s - 1, 0)}, device_id_type=MESH)
    pl.when(s > 0)(lambda: ycopy.start())

    chain_a(4)

    root = z // 4

    def to_even(x2):
        return pltpu.make_async_remote_copy(
            src_ref=fsend.at[x2], dst_ref=frecv.at[xc], send_sem=fsem.at[x2], recv_sem=frsem.at[xc],
            device_id={"gx": 2 * x2}, device_id_type=MESH)

    def to_odd():
        return pltpu.make_async_remote_copy(
            src_ref=bfin, dst_ref=brecv, send_sem=bfsem, recv_sem=bfrsem,
            device_id={"gx": partner}, device_id_type=MESH)

    for i in range(4):
        x2 = (xc + i) % 4
        if i:
            pl.when(core == root)(lambda x2=x2: to_even(x2).start())
        else:
            pl.when((core == root) & (core == 1))(lambda x2=x2: to_even(x2).start())

            @pl.when((core == root) & (core == 0))
            def _():
                frecv[pl.ds(xc, 1)] = fsend[pl.ds(xc, 1)]

    straight_sum()

    @pl.when((root == 0) & (core == 0))
    def _():
        to_odd().start()

    @pl.when((root == 1) & (core == 1))
    def _():
        dw_ref[...] = unpack(bfin[...])

    @pl.when((root == 0) & (core == 1))
    def _():
        to_odd().wait_recv()
        dw_ref[...] = unpack(brecv[...])

    @pl.when(core == 0)
    def _():
        for q in range(4):
            @pl.when((root == 1) | (xc != q))
            def _(q=q):
                pltpu.make_async_remote_copy(
                    src_ref=fsend.at[q], dst_ref=frecv.at[q], send_sem=fsem.at[q], recv_sem=frsem.at[q],
                    device_id={"gx": partner}, device_id_type=MESH).wait_recv()

        dw_ref[...] = unpack((frecv[0] + frecv[1]) + (frecv[2] + frecv[3]))

    for i in range(4):
        x2 = (xc + i) % 4
        if i:
            pl.when(core == root)(lambda x2=x2: to_even(x2).wait_send())
        else:
            pl.when((core == root) & (core == 1))(lambda x2=x2: to_even(x2).wait_send())

    @pl.when((root == 0) & (core == 0))
    def _():
        to_odd().wait_send()

    def drain(j, carry):
        @pl.when((4 * core + j - z + 8) % 8 != 0)
        def _():
            for i in range(4):
                pltpu.make_async_remote_copy(
                    src_ref=sbuf.at[j, i], dst_ref=ra.at[j, i], send_sem=ssem.at[j, i],
                    recv_sem=rasem.at[j, i], device_id={"gy": (z + 1) % 8}, device_id_type=MESH).wait_send()

        return carry

    lax.fori_loop(0, 4, drain, 0)
    for j in range(4):
        pl.when(4 * core + j != z)(lambda j=j: straight(j).wait_send())
    for j in range(4):
        long_in(j).wait_send()
        root_in(j, 1).wait_send()
        root_in(j, 3).wait_send()
    pl.when(s > 0)(lambda: ycopy.wait_send())

    @pl.when(s < 3)
    def _():
        ycopy.wait_recv()
        up_ref[...] = lrecv[...]

    @pl.when(s == 3)
    def _():
        up_ref[...] = jnp.zeros((512, 320), BF16)


def finish(up_in, dw_in, par_in, up_ref, dw_ref, par_ref):
    up_ref[...] = up_in[...]
    dw_ref[...] = dw_in[...].reshape(135, 1, 320)
    par_ref[...] = par_in[...].reshape(3, 1, 320)


def local(level_input, out_grad, conv_weight, norm_gain, norm_shift):
    vm = pl.BlockSpec(memory_space=pltpu.VMEM)
    dma = pltpu.SemaphoreType.DMA
    V = pltpu.VMEM
    up, dw, par = pl.pallas_call(
        kernel,
        out_shape=(V((512, 320), BF16), V((135, 320), F32), V((3, 320), F32)),
        in_specs=[vm, vm, pl.BlockSpec(memory_space=pl.ANY), vm, vm],
        out_specs=(vm, vm, vm),
        scratch_shapes=[
            V((27, 320, 320), BF16), V((3, 6, 160, 320), BF16), V((3, 6, 160, 320), BF16),
            V((4, 3, 128, 128), F32), V((2, 160, 128), F32),
            V((2, 4, 3, 8, 128), F32), V((4, 3, 8, 128), F32), V((4, 3, 8, 128), F32),
            V((2, 2, 3, 8, 128), F32), V((2, 2, 3, 8, 128), F32),
            V((8, 320), F32), V((8, 8, 320), F32), V((8, 320), F32), V((8, 8, 320), F32),
            V((8, 320), F32), V((8, 8, 320), F32), V((8, 320), F32), V((8, 8, 320), F32),
            V((512, 320), BF16), V((512, 320), BF16), V((320, 1024), BF16),
            V((512, 320), F32), V((512, 320), F32), V((512, 320), F32), V((14 * 320 + 8, 320), F32), V((4, 8, 176, 256), F32),
            V((4, 4, 176, 256), BF16), V((4, 4, 176, 256), BF16), V((4, 4, 176, 256), BF16),
            V((4, 176, 256), F32), V((4, 176, 256), BF16), V((8, 176, 256), BF16),
            V((4, 3, 176, 256), BF16), V((4, 176, 256), BF16), V((4, 2, 176, 256), BF16),
            V((4, 176, 256), F32), V((4, 176, 256), F32), V((176, 256), F32), V((176, 256), F32),
            V((512, 320), BF16), V((512, 320), BF16),
            dma(()), dma((2,)), dma((2,)), dma((2,)), dma((2,)), dma((2, 2)), dma((2, 2)), dma(()), dma(()), dma(()), dma(()),
            dma((8,)), dma((8,)), dma((8,)), dma((8,)), dma((8,)), dma((8,)), dma((8,)), dma((8,)),
            dma((4, 4)), dma((4, 4)), dma((4, 4)), dma((4,)), dma((8,)), dma((4, 3)), dma((4,)), dma((4, 2)),
            dma((4,)), dma((4,)), dma(()), dma(()), dma(()), dma(()),
        ],
        compiler_params=pltpu.CompilerParams(
            collective_id=0, has_side_effects=True, vmem_limit_bytes=60 * 1024 * 1024
        ),
    )(
        level_input.reshape(512, 320), out_grad.reshape(4, 128, 320), conv_weight.reshape(27, 320, 320),
        norm_gain, norm_shift,
    )
    up, dw, par = pl.pallas_call(
        finish,
        out_shape=(
            jax.ShapeDtypeStruct((512, 320), BF16),
            jax.ShapeDtypeStruct((135, 1, 320), F32),
            jax.ShapeDtypeStruct((3, 1, 320), F32),
        ),
        in_specs=[vm, vm, vm],
        out_specs=(vm, vm, vm),
        compiler_params=pltpu.CompilerParams(vmem_limit_bytes=8 * 1024 * 1024),
    )(*(pltpu.with_memory_space_constraint(v, pltpu.VMEM) for v in (up, dw, par)))
    return up.reshape(1, 4, 8, 16, 320), dw.reshape(1, 135, 320), par.reshape(1, 3, 320)


def solution(mesh):
    return jax.shard_map(
        local,
        mesh=mesh,
        in_specs=(
            P("section", None, "gy", "gx", None),
            P("section", None, "gy", "gx", None),
            P("section", None, None, None),
            P("section", None),
            P("section", None),
        ),
        out_specs=(
            P("section", None, "gy", "gx", None),
            P("section", ("gy", "gx"), None),
            P("section", None, None),
        ),
        check_vma=False,
    )
```
